256 devices in a mesh: section: 8 (over y, core), expert: 32 (over z, x).
Axes of the slice: x: 4, y: 4, z: 8, core: 2. Of those that a mesh axis runs over, the one named last changes fastest.
Arguments:
- inputs: bfloat16 [8, 4096, 1024], P('section', 'expert'), may hold values from -6 to 6
- out_grads: bfloat16 [8, 4096, 1024], P('section', 'expert'), may hold values from -6 to 6
- expert_ids: int32 [8, 4096, 8], P('section', 'expert'), may hold values from 0 to 63, all different within a row; in each aligned block of 128 rows (0 to 127, 128 to 255, ..., all dimensions but the last counted through in order) at most 24 rows name the same one
- route_levels: int32 [8, 4096, 8], P('section', 'expert'), may hold values from 8 to 256
- w_gate: bfloat16 [8, 64, 1024, 384], P('section', 'expert'), may hold values from -0.1875 to 0.1875
- w_up: bfloat16 [8, 64, 1024, 384], P('section', 'expert'), may hold values from -0.1875 to 0.1875
- w_down: bfloat16 [8, 64, 384, 1024], P('section', 'expert'), may hold values from -0.3125 to 0.3125
Outputs:
- upstream: bfloat16 [8, 4096, 1024], P('section', 'expert')
- route_grad: bfloat16 [8, 4096, 8], P('section', 'expert')
- gate_update: bfloat16 [8, 64, 1024, 384], P('section', 'expert')
- up_update: bfloat16 [8, 64, 1024, 384], P('section', 'expert')
- down_update: bfloat16 [8, 64, 384, 1024], P('section', 'expert')
The draws below stay inside these ranges and needn't reach their ends.
Inputs may be any that keep to these rules, and one draw needn't show every extreme that they name: `expert_ids`: each token names 8 different experts; among the 128 tokens of one aligned block no expert is named more than 24 times.
All inputs are finite; a program needn't handle non-finite values.
Results may differ from the reference program's by a relative error of at most 0.0064.
Values may be sent and summed in bfloat16 or wider, within the bound.
A program may use at most 128 MiB of HBM per device.

```python
import math
import jax
import jax.numpy as jnp
import numpy as np
from jax import lax

D = 1024
H = 384
TOPK = 8
TOK_DEV = 128
EXPERTS = 64
CAP = 24
SECTIONS = 8
TOKENS = 4096
N_EXPERT = 32


def set_ends(entries, own_key, least, high):
    shape = entries.shape
    index_at = [jax.random.randint(jax.random.fold_in(own_key, axis), (), 0, shape[axis]) for axis in range(len(shape))]
    entries = entries.at[tuple(index_at)].set(least)
    longest = shape.index(max(shape))
    index_at[longest] = (index_at[longest] + 1) % shape[longest]
    return entries.at[tuple(index_at)].set(high)


def block_scale(key, extent, split, least, high):
    factor_of = 1.0
    for position, blocks in split:
        heights = jax.random.uniform(jax.random.fold_in(jax.random.fold_in(key, 6), position), (blocks,), jnp.float32, least / len(split), high / len(split))
        factor_of = factor_of * jnp.repeat(jnp.exp(heights), extent[position] // blocks).reshape((-1,) + (1,) * (len(extent) - 1 - position))
    return factor_of


def routed_block(key, own, number, rows, number_of, top, reach, skew):
    ranking = jax.random.permutation(key, number_of)
    crowded, ordinary = shares(number_of, rows * top, reach, skew, True), shares(number_of, rows * top, reach, skew, False)
    places = jnp.arange(number_of)

    def named(sizes, rotation):
        used = int((sizes > 0).sum())
        fixed = max(1, used // 4)
        moved = fixed + (places - fixed + rotation * (used - fixed)) % max(1, number_of - fixed)
        return jnp.zeros((number_of,), jnp.int32).at[ranking[jnp.where(places < fixed, places, moved)]].set(jnp.asarray(sizes, jnp.int32))

    sizes = jnp.where(number % 4 == 0, named(crowded, number // 4), named(ordinary, number - number // 4 - 1))
    mixed = jax.random.permutation(jax.random.fold_in(own, 3), number_of)
    giver, receiver = mixed[0:number_of // 2 * 2:2], mixed[1:number_of // 2 * 2:2]
    room = jnp.minimum(sizes[giver] - 1, reach - sizes[receiver]) // 2
    room = jnp.where((giver == ranking[0]) | (receiver == ranking[0]) | (sizes[receiver] == 0), 0, jnp.maximum(room, 0))
    moved = jax.random.randint(jax.random.fold_in(own, 4), (number_of // 2,), 0, 1 << 20) % (room + 1)
    sizes = sizes.at[giver].add(-moved).at[receiver].add(moved)
    labels = jnp.searchsorted(jnp.cumsum(sizes), jnp.arange(rows * top), side="right").astype(jnp.int32)
    grid = labels.reshape(top, rows).T
    grid = grid[jax.random.permutation(jax.random.fold_in(own, 1), rows)]
    rotation = jax.random.randint(jax.random.fold_in(own, 2), (rows, 1), 0, top)
    return jnp.take_along_axis(grid, (jnp.arange(top)[None, :] + rotation) % top, axis=1)


def shares(number_of, total, reach, skew, full):
    portions = [(1 << 20) // math.isqrt(rank ** skew) + 1 for rank in range(1, number_of + 1)]
    largest = reach if full else min(reach, max(-(-total // number_of), total * portions[0] // sum(portions)))
    least = 1 if total - largest >= number_of - 1 else 0
    counts, spare = [largest] + [least] * (number_of - 1), total - largest - least * (number_of - 1)
    while spare > 0:
        candidates = [i for i in range(1, number_of) if counts[i] < largest] or [i for i in range(1, number_of) if counts[i] < reach]
        pool, budget = sum([portions[i] for i in candidates]), spare
        for i in candidates:
            extra = min(reach - counts[i], max(1, budget * portions[i] // pool), spare)
            counts[i] = counts[i] + extra
            spare = spare - extra
    return np.array(counts)


def gaussian(own_key, extent, deviation, most, cuts=(), kind=jnp.bfloat16):
    factor_of = block_scale(own_key, extent, cuts, -0.22, 0.18) if cuts else 1.0
    array = jax.random.normal(own_key, extent, jnp.float32) * deviation * factor_of
    return jnp.minimum(jnp.maximum(array, -most), most).astype(kind)


def setup_inputs(seed: int = 0) -> dict:
    keys = jax.random.split(jax.random.key(seed), 8)
    inputs = gaussian(keys[0], (SECTIONS, TOKENS, D), 1.0, 6.0, ((0, 8), (1, 32)))
    out_grads = gaussian(keys[1], (SECTIONS, TOKENS, D), 1.0, 6.0, ((0, 8), (1, 32)))
    expert_ids_keys = jax.random.split(jax.random.fold_in(keys[2], 1), SECTIONS * TOKENS // TOK_DEV)
    expert_ids_turns = jax.random.permutation(jax.random.fold_in(keys[2], 3), SECTIONS * TOKENS // TOK_DEV)
    expert_ids = jax.vmap(lambda own, number: routed_block(jax.random.fold_in(keys[2], 2), own, number, TOK_DEV, EXPERTS, TOPK, CAP, 2))(expert_ids_keys, expert_ids_turns).reshape((SECTIONS, TOKENS, TOPK))
    route_levels = set_ends(jax.random.randint(keys[3], (SECTIONS, TOKENS, TOPK), 8, 257), jax.random.fold_in(keys[3], 1), 8, 256).astype(jnp.int32)
    w_gate = gaussian(keys[4], (SECTIONS, EXPERTS, D, H), D ** -0.5, 0.1875, ((0, 8), (1, 32)))
    w_up = gaussian(keys[5], (SECTIONS, EXPERTS, D, H), D ** -0.5, 0.1875, ((0, 8), (1, 32)))
    w_down = gaussian(keys[6], (SECTIONS, EXPERTS, H, D), H ** -0.5, 0.3125, ((0, 8), (1, 32)))
    return {"inputs": inputs, "out_grads": out_grads, "expert_ids": expert_ids, "route_levels": route_levels, "w_gate": w_gate, "w_up": w_up, "w_down": w_down}


def flat_slots(expert_ids, experts_all, capacity):
    blocks = expert_ids.shape[0]
    flat_ids = expert_ids.reshape(blocks, -1).astype(jnp.int32)
    catalog = jnp.arange(experts_all, dtype=jnp.int32)
    onehot = (flat_ids[:, :, None] == catalog[None, None, :]).astype(jnp.int32)
    rank_table = (jnp.cumsum(onehot, axis=1) - 1).astype(jnp.int32)
    slot_of = jnp.sum(onehot * rank_table, axis=2).astype(jnp.int32)
    return (flat_ids * capacity + slot_of).astype(jnp.int32).reshape(expert_ids.shape)


def expert_backward(slot_inputs, slot_grads, slot_routes, w_gate, w_up, w_down):
    inputs_wide = slot_inputs.astype(jnp.float32)
    grads_wide = slot_grads.astype(jnp.float32)
    gate_wide = w_gate.astype(jnp.float32)
    up_wide = w_up.astype(jnp.float32)
    down_wide = w_down.astype(jnp.float32)
    gate_pre = jnp.einsum('esd,edh->esh', inputs_wide, gate_wide)
    up_pre = jnp.einsum('esd,edh->esh', inputs_wide, up_wide)
    sigmoid_gate = jax.nn.sigmoid(gate_pre)
    silu_gate = gate_pre * sigmoid_gate
    active = (silu_gate * up_pre).astype(jnp.bfloat16)
    active_wide = active.astype(jnp.float32)
    expert_out = jnp.einsum('esh,ehd->esd', active_wide, down_wide)
    route_part = jnp.sum(grads_wide * expert_out, axis=2).astype(jnp.bfloat16)
    weighted = (slot_routes.astype(jnp.float32)[:, :, None] * grads_wide).astype(jnp.bfloat16)
    weighted_wide = weighted.astype(jnp.float32)
    active_grad = jnp.einsum('esd,ehd->esh', weighted_wide, down_wide)
    gate_pre_grad = (active_grad * up_pre * sigmoid_gate * (1.0 + gate_pre * (1.0 - sigmoid_gate))).astype(jnp.bfloat16)
    up_pre_grad = (active_grad * silu_gate).astype(jnp.bfloat16)
    gate_grad_wide = gate_pre_grad.astype(jnp.float32)
    up_grad_wide = up_pre_grad.astype(jnp.float32)
    input_grad = (jnp.einsum('esh,edh->esd', gate_grad_wide, gate_wide)
                  + jnp.einsum('esh,edh->esd', up_grad_wide, up_wide)).astype(jnp.bfloat16)
    down_part = jnp.einsum('esh,esd->ehd', active_wide, weighted_wide).astype(jnp.bfloat16)
    gate_part = jnp.einsum('esd,esh->edh', inputs_wide, gate_grad_wide).astype(jnp.bfloat16)
    up_part = jnp.einsum('esd,esh->edh', inputs_wide, up_grad_wide).astype(jnp.bfloat16)
    return input_grad, route_part, gate_part, up_part, down_part


def section_backward(operands):
    inputs, out_grads, expert_ids, route_levels, w_gate, w_up, w_down = operands
    blocks = N_EXPERT
    flat_index = flat_slots(expert_ids.reshape(blocks, TOK_DEV, TOPK), EXPERTS, CAP)
    catalog = jnp.arange(EXPERTS * CAP, dtype=jnp.int32)
    select = (flat_index[..., None] == catalog).astype(jnp.float32).reshape(blocks, TOK_DEV, TOPK, EXPERTS, CAP)
    placing = jnp.sum(select, axis=2)
    route_values = (route_levels.astype(jnp.float32) / 256.0).reshape(blocks, TOK_DEV, TOPK)
    inputs_wide = inputs.astype(jnp.float32).reshape(blocks, TOK_DEV, D)
    grads_wide = out_grads.astype(jnp.float32).reshape(blocks, TOK_DEV, D)
    slot_inputs = jnp.einsum('btec,btd->ebcd', placing, inputs_wide).reshape(EXPERTS, blocks * CAP, D).astype(jnp.bfloat16)
    slot_grads = jnp.einsum('btec,btd->ebcd', placing, grads_wide).reshape(EXPERTS, blocks * CAP, D).astype(jnp.bfloat16)
    slot_routes = jnp.einsum('btkec,btk->ebc', select, route_values).reshape(EXPERTS, blocks * CAP).astype(jnp.bfloat16)
    input_grad, route_part, gate_part, up_part, down_part = expert_backward(slot_inputs, slot_grads, slot_routes, w_gate, w_up, w_down)
    back_inputs = input_grad.astype(jnp.float32).reshape(EXPERTS, blocks, CAP, D)
    token_grad = jnp.einsum('btec,ebcd->btd', placing, back_inputs).reshape(TOKENS, D).astype(jnp.bfloat16)
    back_routes = route_part.astype(jnp.float32).reshape(EXPERTS, blocks, CAP)
    token_route = jnp.einsum('btkec,ebc->btk', select, back_routes).reshape(TOKENS, TOPK).astype(jnp.bfloat16)
    return token_grad, token_route, gate_part, up_part, down_part


def reference(inputs, out_grads, expert_ids, route_levels, w_gate, w_up, w_down):
    token_grad, token_route, gate_part, up_part, down_part = lax.map(
        section_backward, (inputs, out_grads, expert_ids, route_levels, w_gate, w_up, w_down))
    upstream = jnp.concatenate([token_grad[1:], jnp.zeros_like(token_grad[:1])], axis=0)
    return upstream, token_route, gate_part, up_part, down_part
```

```python
import functools

import jax
import jax.numpy as jnp
from jax import lax
from jax.experimental import pallas as pl
from jax.experimental.pallas import tpu as pltpu
from jax.sharding import PartitionSpec as P

NZ = 8
NX = 4
NS = 8
TOK = 128
TOPK = 8
D = 1024
H = 384
EL = 2
CAP = 24
ROW = EL * CAP
ER = EL * NX
ALL = NX * ROW
SRC = NX * CAP
MESH = pl.DeviceIdType.MESH
F32 = jnp.float32
BF16 = jnp.bfloat16


def dot(a, b):
    return jnp.dot(a, b, preferred_element_type=F32)


def dot_t(a, b):
    return lax.dot_general(a, b, (((1,), (1,)), ((), ())), preferred_element_type=F32)


def t_dot(a, b):
    return lax.dot_general(a, b, (((0,), (0,)), ((), ())), preferred_element_type=F32)


def iota(shape, dim):
    return lax.broadcasted_iota(jnp.int32, shape, dim)


def kernel(
    x_in, g_in, ids_in, lev_in, wg_in, wu_in, wd_in,
    up_out, rg_out, gate_out, upw_out, down_out,
    tok, meta, place, sel, got, wgu, wd, xs, ws, act, gug, ret, back, vret, vback,
    part, parts, gpart, gparts, upd, upd_d, ids_t, route_t,
    in_sem, ag_send, ag_recv, mt_send, mt_recv, s_send, s_recv, r_send, r_recv,
    v_send, v_recv, p_send, p_recv, g_send, g_recv, out_sem,
):
    s = lax.axis_index("section")
    e = lax.axis_index("expert")
    z = e // NX
    x = e % NX
    s_prev = (s + NS - 1) % NS
    s_next = (s + 1) % NS

    def device(section, zz, xx):
        return {"section": section, "expert": zz * NX + xx}

    def z_of(i):
        half = (i + 1) // 2
        return (z + NZ + half * (2 * (i % 2) - 1)) % NZ

    def z_from(i):
        half = (i + 1) // 2
        return (z + NZ - half * (2 * (i % 2) - 1)) % NZ

    def remote(src, dst, send, recv, to):
        return pltpu.make_async_remote_copy(
            src_ref=src, dst_ref=dst, send_sem=send, recv_sem=recv, device_id=to, device_id_type=MESH
        )

    own_in = pltpu.make_async_copy(x_in.at[0], tok.at[0, 0], in_sem.at[0])
    own_grad = pltpu.make_async_copy(g_in.at[0], tok.at[0, 1], in_sem.at[1])
    w_copies = [
        pltpu.make_async_copy(wg_in.at[0], wgu.at[:, :, pl.ds(0, H)], in_sem.at[2]),
        pltpu.make_async_copy(wu_in.at[0], wgu.at[:, :, pl.ds(H, H)], in_sem.at[3]),
        pltpu.make_async_copy(wd_in.at[0], wd, in_sem.at[4]),
    ]
    own_in.start()
    own_grad.start()

    barrier = pltpu.get_barrier_semaphore()

    def greet(to):
        pl.semaphore_signal(barrier, inc=1, device_id=to, device_id_type=MESH)

    for k in range(1, NZ):
        greet(device(s, (z + k) % NZ, x))
    for q in range(1, NX):
        greet(device(s, z, (x + q) % NX))
    for k in range(NZ):
        greet(device(s_prev, (z + k) % NZ, x))
        greet(device(s_next, (z + k) % NZ, x))
    for c in w_copies:
        c.start()

    eye = jnp.where(iota((TOK, TOK), 0) == iota((TOK, TOK), 1), 1.0, 0.0).astype(BF16)
    idt = t_dot(ids_in[0].astype(F32).astype(BF16), eye)
    rtt = t_dot(lev_in[0].astype(F32).astype(BF16), eye) / 256.0
    ids_t[...] = idt
    route_t[...] = rtt
    row = iota((TOK, TOK), 0)
    expert_of = ((row // 16) * 8 + row % 8).astype(F32)
    named = jnp.zeros((TOK, TOK), F32)
    route = jnp.zeros((TOK, TOK), F32)
    for k in range(TOPK):
        same = idt[k : k + 1, :] == expert_of
        named = jnp.where(same, 1.0, named)
        route = jnp.where(same, rtt[k : k + 1, :], route)
    before = jnp.where(iota((TOK, TOK), 0) < iota((TOK, TOK), 1), 1.0, 0.0).astype(BF16)
    slot = jnp.where(named > 0.5, dot(named.astype(BF16), before), -1.0)
    meta[0] = jnp.where(row % 16 < 8, slot, route).astype(BF16)

    own_in.wait()
    own_grad.wait()
    pl.semaphore_wait(barrier, (NZ - 1) + (NX - 1) + 2 * NZ)

    def ag(src, dst, h, to):
        return remote(tok.at[src, h], tok.at[dst, h], ag_send.at[dst, h], ag_recv.at[dst, h], to)

    def mt(src, dst, to):
        return remote(meta.at[src], meta.at[dst], mt_send.at[dst], mt_recv.at[dst], to)

    below = device(s, (z + NZ - 1) % NZ, x)
    above = device(s, (z + 1) % NZ, x)

    for h in range(2):
        ag(0, 1, h, below).start()
        ag(0, 2, h, above).start()
    mt(0, 1, below).start()
    mt(0, 2, above).start()

    def select(i):
        def forward():
            @pl.when(i < NZ)
            def _():
                mt(i, i, above).wait_recv()
                for h in range(2):
                    ag(i, i, h, above).wait_recv()

            to = device(s, (z + NZ + 1 - 2 * (i % 2)) % NZ, x)

            @pl.when(i < NZ - 3)
            def _():
                for h in range(2):
                    ag(i, i + 2, h, to).start()
                mt(i, i + 2, to).start()

            @pl.when(i == NZ - 3)
            def _():
                ag(NZ - 3, NZ - 1, 1, to).start()

            @pl.when(i == NZ - 2)
            def _():
                ag(NZ - 2, NZ - 1, 0, to).start()
                mt(NZ - 2, NZ - 1, to).start()

        pl.when(i > 0)(forward)

        group = meta[i, pl.ds(pl.multiple_of(z * 16, 16), 16), :].astype(F32)
        place_of = iota((CAP, TOK), 0).astype(F32)
        ones, routes = [], []
        for k in range(ER):
            hit = group[k : k + 1, :] == place_of
            ones.append(jnp.where(hit, 1.0, 0.0))
            routes.append(jnp.where(hit, group[ER + k : ER + k + 1, :], 0.0))
        one = jnp.concatenate(ones, axis=0).astype(BF16)
        weight = jnp.concatenate(routes, axis=0).astype(BF16)
        place[i] = one
        for h, chosen in ((0, one), (1, weight)):
            for n in range(0, D, 256):
                rows = dot(chosen, tok[i, h, :, n : n + 256]).astype(BF16)
                for q in range(NX):
                    sel[i, q, h, :, n : n + 256] = rows[q * ROW : (q + 1) * ROW]
        for q in range(1, NX):
            xx = (x + q) % NX
            sent(i, xx).start()
        got[i, x] = sel[i, x]

    def sent(i, xx):
        return remote(sel.at[i, xx], got.at[i, x], s_send.at[i, xx], s_recv.at[i, x], device(s, z, xx))

    def arrived(i, xx):
        return remote(sel.at[i, x], got.at[i, xx], s_send.at[i, xx], s_recv.at[i, xx], device(s, z, xx))

    def returned(i, xx):
        return remote(ret.at[i, xx], back.at[i, x], r_send.at[i, xx], r_recv.at[i, x], device(s, z, xx))

    def came_back(i, xx):
        return remote(ret.at[i, x], back.at[i, xx], r_send.at[i, xx], r_recv.at[i, xx], device(s, z, xx))

    def v_returned(i, xx):
        return remote(vret.at[i], vback.at[i, x], v_send.at[i, xx], v_recv.at[i, x], device(s, z, xx))

    def v_came_back(i, xx):
        return remote(vret.at[i], vback.at[i, xx], v_send.at[i, xx], v_recv.at[i, xx], device(s, z, xx))

    def expert_rows(i):
        for q in range(1, NX):
            arrived(i, (x + q) % NX).wait_recv()
        at = pl.ds(pl.multiple_of(i * SRC, 32), SRC)
        wide = [got[i, q, 0].astype(F32) for q in range(NX)]
        wide_w = [got[i, q, 1].astype(F32) for q in range(NX)]
        grads, vs = [], []
        for k in range(EL):
            mine = slice(k * CAP, (k + 1) * CAP)
            rows = jnp.concatenate([w[mine] for w in wide], axis=0).astype(BF16)
            weighted = jnp.concatenate([w[mine] for w in wide_w], axis=0).astype(BF16)
            xs[k, at, :] = rows
            ws[k, at, :] = weighted
            pre = dot(rows, wgu[k])
            gate, up = pre[:, :H], pre[:, H:]
            active_grad = dot_t(weighted, wd[k])
            sig = jax.nn.sigmoid(gate)
            silu = gate * sig
            active = (silu * up).astype(BF16)
            gate_grad = (active_grad * up * sig * (1.0 + gate * (1.0 - sig))).astype(BF16)
            up_grad = (active_grad * silu).astype(BF16)
            act[k, at, :] = active
            gug[k, at, 0:H] = gate_grad
            gug[k, at, H : 2 * H] = up_grad
            vs.append(jnp.sum(active.astype(F32) * active_grad, axis=1, keepdims=True))
            grads.append(jnp.concatenate([gate_grad, up_grad], axis=1))
        for n in range(0, D, 256):
            outs = [dot_t(grads[k], wgu[k, n : n + 256, :]) for k in range(EL)]
            for q in range(NX):
                piece = jnp.concatenate([o[q * CAP : (q + 1) * CAP] for o in outs], axis=0)
                ret[i, q, :, n : n + 256] = piece.astype(BF16)
        lines = []
        for q in range(NX):
            line = jnp.zeros((1, TOK), F32)
            for k in range(EL):
                at_lane = iota((CAP, TOK), 1) == iota((CAP, TOK), 0) + k * CAP
                line += jnp.sum(
                    jnp.where(at_lane, vs[k][q * CAP : (q + 1) * CAP], 0.0), axis=0, keepdims=True
                )
            lines.append(line)
        lines.append(jnp.zeros((8 - NX, TOK), F32))
        vret[i] = jnp.concatenate(lines, axis=0)
        for q in range(1, NX):
            xx = (x + q) % NX
            returned(i, xx).start()
            v_returned(i, xx).start()
        back[i, x] = ret[i, x]
        vback[i, x] = vret[i]

    def summed(i):
        return remote(part.at[i], parts.at[i], p_send.at[i], p_recv.at[i], device(s_prev, z_of(i), x))

    def g_summed(i):
        return remote(gpart.at[i], gparts.at[i], g_send.at[i], g_recv.at[i], device(s, z_of(i), x))

    def combine(i):
        for q in range(1, NX):
            came_back(i, (x + q) % NX).wait_recv()
            v_came_back(i, (x + q) % NX).wait_recv()
        one = place[i]
        for n in range(0, D, 256):
            rows = back[i, :, :, n : n + 256].reshape(ALL, 256)
            part[i, :, n : n + 256] = t_dot(one, rows).astype(BF16)
        summed(i).start()
        lines = []
        for q in range(NX):
            line = vback[i, q, pl.ds(x, 1), :]
            at_lane = iota((ROW, TOK), 1) == iota((ROW, TOK), 0)
            column = jnp.sum(jnp.where(at_lane, line, 0.0), axis=1, keepdims=True)
            spread = one[q * ROW : (q + 1) * ROW].astype(F32) * column
            for k in range(EL):
                lines.append(jnp.sum(spread[k * CAP : (k + 1) * CAP], axis=0, keepdims=True))
        gpart[i] = jnp.concatenate(lines, axis=0)

        @pl.when(i > 0)
        def _():
            g_summed(i).start()

        @pl.when(i == 0)
        def _():
            gparts[0] = gpart[0]

    def update(k):
        for m in range(0, D, 256):
            new = t_dot(xs[k, :, m : m + 256], gug[k])
            upd[k, 0, m : m + 256, :] = new[:, :H].astype(BF16)
            upd[k, 1, m : m + 256, :] = new[:, H:].astype(BF16)
        upd_d[k] = t_dot(act[k], ws[k]).astype(BF16)
        for c in outs_of(k):
            c.start()

    def outs_of(k):
        return [
            pltpu.make_async_copy(upd.at[k, 0], gate_out.at[0, k], out_sem.at[k, 0]),
            pltpu.make_async_copy(upd.at[k, 1], upw_out.at[0, k], out_sem.at[k, 1]),
            pltpu.make_async_copy(upd_d.at[k], down_out.at[0, k], out_sem.at[k, 2]),
        ]

    def step(t, carry):
        @pl.when(t < NZ)
        def _():
            select(t)

        @pl.when(t == 2)
        def _():
            for c in w_copies:
                c.wait()

        @pl.when(t >= 2)
        def _():
            expert_rows(t - 2)

        @pl.when(t >= 4)
        def _():
            combine(t - 4)

        return carry

    lax.fori_loop(0, NZ + 2, step, 0)
    combine(NZ - 2)
    update(0)
    combine(NZ - 1)
    update(1)

    for i in range(1, NZ):
        g_summed(i).wait_recv()
    acc = jnp.zeros((TOPK, TOK), F32)
    idt = ids_t[...]
    for i in range(NZ):
        base = z_from(i) * ER
        for k in range(ER):
            acc += jnp.where(idt == (base + k).astype(F32), gparts[i, k : k + 1, :], 0.0)
    final = (acc / route_t[...]).astype(BF16).astype(F32)
    square = jnp.concatenate([final, jnp.zeros((TOK - TOPK, TOK), F32)], axis=0).astype(BF16)
    rg_out[0] = dot_t(eye, square)[:, :TOPK].astype(BF16)

    total = None
    for i in range(NZ):
        summed(i).wait_recv()
        term = parts[i].astype(F32)
        total = term if total is None else total + term
    up_out[0] = jnp.where(s == NS - 1, 0.0, total).astype(BF16)

    def drain(i, carry):
        @pl.when(i > 0)
        def _():
            @pl.when(i < NZ)
            def _():
                mt(0, i, above).wait_send()
                for h in range(2):
                    ag(0, i, h, above).wait_send()

            g_summed(i).wait_send()

        for q in range(1, NX):
            xx = (x + q) % NX
            sent(i, xx).wait_send()
            returned(i, xx).wait_send()
            v_returned(i, xx).wait_send()
        summed(i).wait_send()
        return carry

    lax.fori_loop(0, NZ, drain, 0)
    for k in range(EL):
        for c in outs_of(k):
            c.wait()


def body(inputs, out_grads, expert_ids, route_levels, w_gate, w_up, w_down):
    any_spec = pl.BlockSpec(memory_space=pl.ANY)
    vmem = pl.BlockSpec(memory_space=pltpu.VMEM)
    dma = pltpu.SemaphoreType.DMA
    flops = 2 * 8 * EL * NZ * SRC * D * H
    return pl.pallas_call(
        kernel,
        name="layer_backward",
        out_shape=(
            jax.ShapeDtypeStruct((1, TOK, D), BF16),
            jax.ShapeDtypeStruct((1, TOK, TOPK), BF16),
            jax.ShapeDtypeStruct((1, EL, D, H), BF16),
            jax.ShapeDtypeStruct((1, EL, D, H), BF16),
            jax.ShapeDtypeStruct((1, EL, H, D), BF16),
        ),
        in_specs=[any_spec, any_spec, vmem, vmem, any_spec, any_spec, any_spec],
        out_specs=(vmem, vmem, any_spec, any_spec, any_spec),
        scratch_shapes=[
            pltpu.VMEM((NZ, 2, TOK, D), BF16),
            pltpu.VMEM((NZ, TOK, TOK), BF16),
            pltpu.VMEM((NZ, ALL, TOK), BF16),
            pltpu.VMEM((NZ, NX, 2, ROW, D), BF16),
            pltpu.VMEM((NZ, NX, 2, ROW, D), BF16),
            pltpu.VMEM((EL, D, 2 * H), BF16),
            pltpu.VMEM((EL, H, D), BF16),
            pltpu.VMEM((EL, NZ * SRC, D), BF16),
            pltpu.VMEM((EL, NZ * SRC, D), BF16),
            pltpu.VMEM((EL, NZ * SRC, H), BF16),
            pltpu.VMEM((EL, NZ * SRC, 2 * H), BF16),
            pltpu.VMEM((NZ, NX, ROW, D), BF16),
            pltpu.VMEM((NZ, NX, ROW, D), BF16),
            pltpu.VMEM((NZ, 8, TOK), F32),
            pltpu.VMEM((NZ, NX, 8, TOK), F32),
            pltpu.VMEM((NZ, TOK, D), BF16),
            pltpu.VMEM((NZ, TOK, D), BF16),
            pltpu.VMEM((NZ, ER, TOK), F32),
            pltpu.VMEM((NZ, ER, TOK), F32),
            pltpu.VMEM((EL, 2, D, H), BF16),
            pltpu.VMEM((EL, H, D), BF16),
            pltpu.VMEM((TOPK, TOK), F32),
            pltpu.VMEM((TOPK, TOK), F32),
            dma((5,)),
            dma((NZ, 2)),
            dma((NZ, 2)),
            dma((NZ,)),
            dma((NZ,)),
            dma((NZ, NX)),
            dma((NZ, NX)),
            dma((NZ, NX)),
            dma((NZ, NX)),
            dma((NZ, NX)),
            dma((NZ, NX)),
            dma((NZ,)),
            dma((NZ,)),
            dma((NZ,)),
            dma((NZ,)),
            dma((EL, 3)),
        ],
        compiler_params=pltpu.CompilerParams(
            collective_id=0, has_side_effects=True, vmem_limit_bytes=60 * 1024 * 1024
        ),
        cost_estimate=pl.CostEstimate(flops=flops, bytes_accessed=12 << 20, transcendentals=EL * NZ * SRC * H),
    )(inputs, out_grads, expert_ids, route_levels, w_gate, w_up, w_down)


def solution(mesh):
    rows = P("section", "expert", None)
    experts = P("section", "expert", None, None)
    return jax.shard_map(
        body,
        mesh=mesh,
        in_specs=(rows, rows, rows, rows, experts, experts, experts),
        out_specs=(rows, rows, experts, experts, experts),
        check_vma=False,
    )
```

```python
import jax
import jax.numpy as jnp
from jax import lax
from jax.experimental import pallas as pl
from jax.experimental.pallas import tpu as pltpu
from jax.sharding import PartitionSpec as P

NZ = 8
NX = 4
NS = 8
TOK = 128
TOPK = 8
D = 1024
H = 384
EL = 2
CAP = 24
ROW = EL * CAP
ER = EL * NX
ALL = NX * ROW
SRC = NX * CAP
AWAY = (0, 1, -1, 2, -2, 3, -3, 4)
MESH = pl.DeviceIdType.MESH
F32 = jnp.float32
BF16 = jnp.bfloat16


def dot(a, b):
    return jnp.dot(a, b, preferred_element_type=F32)


def dot_t(a, b):
    return lax.dot_general(a, b, (((1,), (1,)), ((), ())), preferred_element_type=F32)


def t_dot(a, b):
    return lax.dot_general(a, b, (((0,), (0,)), ((), ())), preferred_element_type=F32)


def iota(shape, dim):
    return lax.broadcasted_iota(jnp.int32, shape, dim)


def kernel(
    x_in, g_in, ids_in, lev_in, wg_in, wu_in, wd_in,
    up_out, rg_out, gate_out, upw_out, down_out,
    tok, meta, place, place_w, sel, got, wgu, wd, xs, ws, act, gug, ret, back, vret, vback,
    part, inc, fin, gpart, gparts, upd, upd_d,
    in_sem, ag_send, ag_recv, mt_send, mt_recv, s_send, s_recv, r_send, r_recv,
    v_send, v_recv, p_send, p_recv, f_send, f_recv, g_send, g_recv, out_sem,
):
    s = lax.axis_index("section")
    e = lax.axis_index("expert")
    z = e // NX
    x = e % NX
    s_prev = (s + NS - 1) % NS
    s_next = (s + 1) % NS
    others = [(x + q) % NX for q in range(1, NX)]

    def device(section, zz, xx):
        return {"section": section, "expert": ((zz + NZ) % NZ) * NX + xx}

    below, above = device(s, z - 1, x), device(s, z + 1, x)

    def remote(src, dst, send, recv, to):
        return pltpu.make_async_remote_copy(
            src_ref=src, dst_ref=dst, send_sem=send, recv_sem=recv, device_id=to, device_id_type=MESH
        )

    def ag(src, dst, h, to):
        return remote(tok.at[src, h], tok.at[dst, h], ag_send.at[dst, h], ag_recv.at[dst, h], to)

    def mt(src, dst, to):
        return remote(meta.at[src], meta.at[dst], mt_send.at[dst], mt_recv.at[dst], to)

    def sent(i, h, xx):
        return remote(
            sel.at[i, xx, h], got.at[i, x, h], s_send.at[i, xx, h], s_recv.at[i, x, h], device(s, z, xx)
        )

    def arrived(i, h, xx):
        return remote(
            sel.at[i, x, h], got.at[i, xx, h], s_send.at[i, xx, h], s_recv.at[i, xx, h], device(s, z, xx)
        )

    def returned(i, xx):
        return remote(ret.at[i, xx], back.at[i, x], r_send.at[i, xx], r_recv.at[i, x], device(s, z, xx))

    def came_back(i, xx):
        return remote(ret.at[i, x], back.at[i, xx], r_send.at[i, xx], r_recv.at[i, xx], device(s, z, xx))

    def v_returned(i, xx):
        return remote(vret.at[i], vback.at[i, x], v_send.at[i, xx], v_recv.at[i, x], device(s, z, xx))

    def v_came_back(i, xx):
        return remote(vret.at[i], vback.at[i, xx], v_send.at[i, xx], v_recv.at[i, xx], device(s, z, xx))

    def onward(i):
        if i == 7:
            low, high = pl.ds(0, D // 2), pl.ds(D // 2, D // 2)
            return [
                remote(part.at[7, :, low], inc.at[5, :, low], p_send.at[5], p_recv.at[5], above),
                remote(part.at[7, :, high], inc.at[6, :, high], p_send.at[6], p_recv.at[6], below),
            ]
        if i > 2:
            to = above if i % 2 else below
            return [remote(part.at[i], inc.at[i - 2], p_send.at[i - 2], p_recv.at[i - 2], to)]
        to = device(s_prev, z + AWAY[i], x)
        return [remote(part.at[i], fin.at[i], f_send.at[i], f_recv.at[i], to)]

    def incoming(i):
        return onward(7)[i - 5] if i > 4 else onward(i + 2)[0]

    def g_summed(i):
        return remote(gpart.at[i], gparts.at[i], g_send.at[i], g_recv.at[i], device(s, z + AWAY[i], x))

    own_in = pltpu.make_async_copy(x_in.at[0], tok.at[0, 0], in_sem.at[0])
    own_grad = pltpu.make_async_copy(g_in.at[0], tok.at[0, 1], in_sem.at[1])
    w_copies = [
        pltpu.make_async_copy(wg_in.at[0], wgu.at[:, :, pl.ds(0, H)], in_sem.at[2]),
        pltpu.make_async_copy(wu_in.at[0], wgu.at[:, :, pl.ds(H, H)], in_sem.at[3]),
        pltpu.make_async_copy(wd_in.at[0], wd, in_sem.at[4]),
    ]
    own_in.start()
    own_grad.start()

    barrier = pltpu.get_barrier_semaphore()

    def greet(to):
        pl.semaphore_signal(barrier, inc=1, device_id=to, device_id_type=MESH)

    for k in range(1, NZ):
        greet(device(s, z + k, x))
    for xx in others:
        greet(device(s, z, xx))
    for k in (-1, 0, 1):
        greet(device(s_prev, z + k, x))
        greet(device(s_next, z + k, x))
    for c in w_copies:
        c.start()

    idt = ids_in[0].astype(F32)
    rtt = lev_in[0].astype(F32) / 256.0
    row = iota((TOK, TOK), 0)
    expert_of = ((row // 16) * 8 + row % 8).astype(F32)
    named = jnp.zeros((TOK, TOK), F32)
    route = jnp.zeros((TOK, TOK), F32)
    for k in range(TOPK):
        same = idt[k : k + 1, :] == expert_of
        named = jnp.where(same, 1.0, named)
        route = jnp.where(same, rtt[k : k + 1, :], route)
    before = jnp.where(iota((TOK, TOK), 0) < iota((TOK, TOK), 1), 1.0, 0.0).astype(BF16)
    slot = jnp.where(named > 0.5, dot(named.astype(BF16), before), -1.0)
    meta[0] = jnp.where(row % 16 < 8, slot, route).astype(BF16)

    def places(i):
        group = meta[i, pl.ds(pl.multiple_of(z * 16, 16), 16), :].astype(F32)
        place_of = iota((CAP, TOK), 0).astype(F32)
        ones, routes = [], []
        for k in range(ER):
            hit = group[k : k + 1, :] == place_of
            ones.append(jnp.where(hit, 1.0, 0.0))
            routes.append(jnp.where(hit, group[ER + k : ER + k + 1, :], 0.0))
        place[i] = jnp.concatenate(ones, axis=0).astype(BF16)
        place_w[i] = jnp.concatenate(routes, axis=0).astype(BF16)

    def chosen(i, h):
        if h == 0:
            places(i)
        which = place_w[i] if h else place[i]
        for n in range(0, D, 256):
            rows = dot(which, tok[i, h, :, n : n + 256]).astype(BF16)
            for q in range(NX):
                sel[i, q, h, :, n : n + 256] = rows[q * ROW : (q + 1) * ROW]

    def send_chosen(i, h):
        for xx in others:
            sent(i, h, xx).start()
        got[i, x, h] = sel[i, x, h]

    def pass_on(i, h):
        if h == 0:
            mt(i, i, above).wait_recv()
        ag(i, i, h, above).wait_recv()
        if i == 7 or (i == 5 and h == 0) or (i == 6 and h == 1):
            return
        to, dst = (below, above)[1 - i % 2], min(i + 2, 7)
        if h == 0:
            mt(i, dst, to).start()
        ag(i, dst, h, to).start()

    def select(i, h):
        chosen(i, h)
        send_chosen(i, h)

    def expert_rows(i):
        for xx in others:
            for h in range(2):
                arrived(i, h, xx).wait_recv()
        at = slice(i * SRC, (i + 1) * SRC)
        wide = [got[i, q, 0].astype(F32) for q in range(NX)]
        wide_w = [got[i, q, 1].astype(F32) for q in range(NX)]
        grads, vs = [], []
        for k in range(EL):
            mine = slice(k * CAP, (k + 1) * CAP)
            rows = jnp.concatenate([w[mine] for w in wide], axis=0).astype(BF16)
            weighted = jnp.concatenate([w[mine] for w in wide_w], axis=0).astype(BF16)
            xs[k, at, :] = rows
            ws[k, at, :] = weighted
            pre = dot(rows, wgu[k])
            gate, up = pre[:, :H], pre[:, H:]
            active_grad = dot_t(weighted, wd[k])
            sig = jax.nn.sigmoid(gate)
            silu = gate * sig
            active = (silu * up).astype(BF16)
            gate_grad = (active_grad * up * sig * (1.0 + gate * (1.0 - sig))).astype(BF16)
            up_grad = (active_grad * silu).astype(BF16)
            act[k, at, :] = active
            gug[k, at, 0:H] = gate_grad
            gug[k, at, H : 2 * H] = up_grad
            vs.append(jnp.sum(active.astype(F32) * active_grad, axis=1, keepdims=True))
            grads.append(jnp.concatenate([gate_grad, up_grad], axis=1))
        for n in range(0, D, 256):
            outs = [dot_t(grads[k], wgu[k, n : n + 256, :]) for k in range(EL)]
            for q in range(NX):
                piece = jnp.concatenate([o[q * CAP : (q + 1) * CAP] for o in outs], axis=0)
                ret[i, q, :, n : n + 256] = piece.astype(BF16)
        lines = []
        for q in range(NX):
            line = jnp.zeros((1, TOK), F32)
            for k in range(EL):
                at_lane = iota((CAP, TOK), 1) == iota((CAP, TOK), 0) + k * CAP
                line += jnp.sum(
                    jnp.where(at_lane, vs[k][q * CAP : (q + 1) * CAP], 0.0), axis=0, keepdims=True
                )
            lines.append(line)
        lines.append(jnp.zeros((8 - NX, TOK), F32))
        vret[i] = jnp.concatenate(lines, axis=0)
        back[i, x] = ret[i, x]
        vback[i, x] = vret[i]

    def send_back(i):
        for xx in others:
            returned(i, xx).start()
            v_returned(i, xx).start()

    def combine(i):
        for xx in others:
            came_back(i, xx).wait_recv()
            v_came_back(i, xx).wait_recv()
        if 0 < i < 7:
            incoming(i).wait_recv()
        one = place[i]
        for n in range(0, D, 256):
            rows = back[i, :, :, n : n + 256].reshape(ALL, 256)
            total = t_dot(one, rows)
            if 0 < i < 5 or (i == 5 and n < D // 2) or (i == 6 and n >= D // 2):
                total += inc[i, :, n : n + 256].astype(F32)
            part[i, :, n : n + 256] = total.astype(BF16)
        for c in onward(i):
            c.start()
        lines = []
        for q in range(NX):
            line = vback[i, q, pl.ds(x, 1), :]
            at_lane = iota((ROW, TOK), 1) == iota((ROW, TOK), 0)
            column = jnp.sum(jnp.where(at_lane, line, 0.0), axis=1, keepdims=True)
            spread = one[q * ROW : (q + 1) * ROW].astype(F32) * column
            for k in range(EL):
                lines.append(jnp.sum(spread[k * CAP : (k + 1) * CAP], axis=0, keepdims=True))
        summed = jnp.concatenate(lines, axis=0)
        if i:
            gpart[i] = summed
            g_summed(i).start()
        else:
            gparts[0] = summed

    def outs_of(k):
        return [
            pltpu.make_async_copy(upd.at[k, 0], gate_out.at[0, k], out_sem.at[k, 0]),
            pltpu.make_async_copy(upd.at[k, 1], upw_out.at[0, k], out_sem.at[k, 1]),
            pltpu.make_async_copy(upd_d.at[k], down_out.at[0, k], out_sem.at[k, 2]),
        ]

    def update(k, stage):
        if stage < 2:
            for m in range(stage * D // 2, (stage + 1) * D // 2, 256):
                new = t_dot(xs[k, :, m : m + 256], gug[k])
                upd[k, 0, m : m + 256, :] = new[:, :H].astype(BF16)
                upd[k, 1, m : m + 256, :] = new[:, H:].astype(BF16)
        else:
            upd_d[k] = t_dot(act[k], ws[k]).astype(BF16)
            for c in outs_of(k):
                c.start()

    own_in.wait()
    own_grad.wait()
    chosen(0, 0)
    chosen(0, 1)
    pl.semaphore_wait(barrier, (NZ - 1) + (NX - 1) + 6)
    mt(0, 1, below).start()
    mt(0, 2, above).start()
    for h in range(2):
        ag(0, 1, h, below).start()
        ag(0, 2, h, above).start()
        send_chosen(0, h)

    def both(a, b, h):
        pass_on(a, h)
        pass_on(b, h)
        select(a, h)
        select(b, h)

    both(1, 2, 0)
    both(1, 2, 1)
    for c in w_copies:
        c.wait()
    expert_rows(0)
    both(3, 4, 0)
    expert_rows(1)
    both(3, 4, 1)
    expert_rows(2)
    both(5, 6, 0)
    expert_rows(3)
    pass_on(5, 1)
    pass_on(6, 1)
    select(5, 1)
    pass_on(7, 0)
    pass_on(7, 1)
    select(7, 0)
    select(7, 1)
    select(6, 1)
    expert_rows(4)
    expert_rows(5)
    expert_rows(7)
    send_back(7)
    send_back(5)
    expert_rows(6)
    for i in (6, 3, 4, 1, 2, 0):
        send_back(i)
    combine(7)
    update(0, 0)
    combine(5)
    update(0, 1)
    combine(6)
    update(0, 2)
    combine(3)
    update(1, 0)
    combine(4)
    update(1, 1)
    combine(1)
    update(1, 2)
    combine(2)
    combine(0)

    for i in range(1, NZ):
        g_summed(i).wait_recv()
    acc = jnp.zeros((TOPK, TOK), F32)
    idt = ids_in[0].astype(F32)
    for i in range(NZ):
        base = ((z + NZ - AWAY[i]) % NZ) * ER
        for k in range(ER):
            acc += jnp.where(idt == (base + k).astype(F32), gparts[i, k : k + 1, :], 0.0)
    rg_out[0] = (acc / (lev_in[0].astype(F32) / 256.0)).astype(BF16)

    for i in range(3):
        onward(i)[0].wait_recv()
    total = fin[0].astype(F32) + fin[1].astype(F32) + fin[2].astype(F32)
    up_out[0] = jnp.where(s == NS - 1, 0.0, total).astype(BF16)

    for i in range(NZ):
        if i:
            mt(0, i, above).wait_send()
            for h in range(2):
                ag(0, i, h, above).wait_send()
            g_summed(i).wait_send()
        for xx in others:
            for h in range(2):
                sent(i, h, xx).wait_send()
            returned(i, xx).wait_send()
            v_returned(i, xx).wait_send()
        for c in onward(i):
            c.wait_send()
    for k in range(EL):
        for c in outs_of(k):
            c.wait()


def body(inputs, out_grads, expert_ids, route_levels, w_gate, w_up, w_down):
    any_spec = pl.BlockSpec(memory_space=pl.ANY)
    vmem = pl.BlockSpec(memory_space=pltpu.VMEM)
    dma = pltpu.SemaphoreType.DMA
    flops = 2 * 8 * EL * NZ * SRC * D * H
    upstream, route_grad, *updates = pl.pallas_call(
        kernel,
        name="layer_backward",
        out_shape=(
            jax.ShapeDtypeStruct((1, TOK, D), BF16),
            jax.ShapeDtypeStruct((1, TOPK, TOK), BF16),
            jax.ShapeDtypeStruct((1, EL, D, H), BF16),
            jax.ShapeDtypeStruct((1, EL, D, H), BF16),
            jax.ShapeDtypeStruct((1, EL, H, D), BF16),
        ),
        in_specs=[any_spec, any_spec, vmem, vmem, any_spec, any_spec, any_spec],
        out_specs=(vmem, vmem, any_spec, any_spec, any_spec),
        scratch_shapes=[
            pltpu.VMEM((NZ, 2, TOK, D), BF16),
            pltpu.VMEM((NZ, TOK, TOK), BF16),
            pltpu.VMEM((NZ, ALL, TOK), BF16),
            pltpu.VMEM((NZ, ALL, TOK), BF16),
            pltpu.VMEM((NZ, NX, 2, ROW, D), BF16),
            pltpu.VMEM((NZ, NX, 2, ROW, D), BF16),
            pltpu.VMEM((EL, D, 2 * H), BF16),
            pltpu.VMEM((EL, H, D), BF16),
            pltpu.VMEM((EL, NZ * SRC, D), BF16),
            pltpu.VMEM((EL, NZ * SRC, D), BF16),
            pltpu.VMEM((EL, NZ * SRC, H), BF16),
            pltpu.VMEM((EL, NZ * SRC, 2 * H), BF16),
            pltpu.VMEM((NZ, NX, ROW, D), BF16),
            pltpu.VMEM((NZ, NX, ROW, D), BF16),
            pltpu.VMEM((NZ, 8, TOK), F32),
            pltpu.VMEM((NZ, NX, 8, TOK), F32),
            pltpu.VMEM((NZ, TOK, D), BF16),
            pltpu.VMEM((NZ, TOK, D), BF16),
            pltpu.VMEM((3, TOK, D), BF16),
            pltpu.VMEM((NZ, ER, TOK), F32),
            pltpu.VMEM((NZ, ER, TOK), F32),
            pltpu.VMEM((EL, 2, D, H), BF16),
            pltpu.VMEM((EL, H, D), BF16),
            dma((5,)),
            dma((NZ, 2)),
            dma((NZ, 2)),
            dma((NZ,)),
            dma((NZ,)),
            dma((NZ, NX, 2)),
            dma((NZ, NX, 2)),
            dma((NZ, NX)),
            dma((NZ, NX)),
            dma((NZ, NX)),
            dma((NZ, NX)),
            dma((NZ,)),
            dma((NZ,)),
            dma((3,)),
            dma((3,)),
            dma((NZ,)),
            dma((NZ,)),
            dma((EL, 3)),
        ],
        compiler_params=pltpu.CompilerParams(
            collective_id=0, has_side_effects=True, vmem_limit_bytes=60 * 1024 * 1024
        ),
        cost_estimate=pl.CostEstimate(flops=flops, bytes_accessed=12 << 20, transcendentals=EL * NZ * SRC * H),
    )(inputs, out_grads, jnp.swapaxes(expert_ids, 1, 2), jnp.swapaxes(route_levels, 1, 2), w_gate, w_up, w_down)
    return (upstream, jnp.swapaxes(route_grad, 1, 2), *updates)


def solution(mesh):
    rows = P("section", "expert", None)
    experts = P("section", "expert", None, None)
    return jax.shard_map(
        body,
        mesh=mesh,
        in_specs=(rows, rows, rows, rows, experts, experts, experts),
        out_specs=(rows, rows, experts, experts, experts),
        check_vma=False,
    )
```

```python
import jax
import jax.numpy as jnp
from jax import lax
from jax.experimental import pallas as pl
from jax.experimental.pallas import tpu as pltpu
from jax.sharding import PartitionSpec as P

NZ = 8
NX = 4
NS = 8
TOK = 128
TOPK = 8
D = 1024
H = 384
EL = 2
CAP = 24
ROW = EL * CAP
ER = EL * NX
ALL = NX * ROW
SRC = NX * CAP
AWAY = (0, 1, -1, 2, -2, 3, -3, 4)
MESH = pl.DeviceIdType.MESH
F32 = jnp.float32
BF16 = jnp.bfloat16


def dot(a, b):
    return jnp.dot(a, b, preferred_element_type=F32)


def dot_t(a, b):
    return lax.dot_general(a, b, (((1,), (1,)), ((), ())), preferred_element_type=F32)


def t_dot(a, b):
    return lax.dot_general(a, b, (((0,), (0,)), ((), ())), preferred_element_type=F32)


def iota(shape, dim):
    return lax.broadcasted_iota(jnp.int32, shape, dim)


def kernel(
    x_in, g_in, ids_in, lev_in, wg_in, wu_in, wd_in,
    up_out, rg_out, gate_out, upw_out, down_out,
    tok, meta, place, place_w, sel, got, wgu, wd, xs, ws, act, gug, ret, back, vret, vback,
    part, inc, fin, gpart, gparts,
    in_sem, ag_send, ag_recv, mt_send, mt_recv, s_send, s_recv, r_send, r_recv,
    v_send, v_recv, p_send, p_recv, f_send, f_recv, g_send, g_recv,
):
    s = lax.axis_index("section")
    e = lax.axis_index("expert")
    z = e // NX
    x = e % NX
    s_prev = (s + NS - 1) % NS
    s_next = (s + 1) % NS
    others = [(x + q) % NX for q in range(1, NX)]

    def device(section, zz, xx):
        return {"section": section, "expert": ((zz + NZ) % NZ) * NX + xx}

    below, above = device(s, z - 1, x), device(s, z + 1, x)

    def remote(src, dst, send, recv, to):
        return pltpu.make_async_remote_copy(
            src_ref=src, dst_ref=dst, send_sem=send, recv_sem=recv, device_id=to, device_id_type=MESH
        )

    def ag(src, dst, h, to):
        return remote(tok.at[src, h], tok.at[dst, h], ag_send.at[dst, h], ag_recv.at[dst, h], to)

    def mt(src, dst, to):
        return remote(meta.at[src], meta.at[dst], mt_send.at[dst], mt_recv.at[dst], to)

    def sent(i, h, xx):
        return remote(
            sel.at[i, xx, h], got.at[i, x, h], s_send.at[i, xx, h], s_recv.at[i, x, h], device(s, z, xx)
        )

    def arrived(i, h, xx):
        return remote(
            sel.at[i, x, h], got.at[i, xx, h], s_send.at[i, xx, h], s_recv.at[i, xx, h], device(s, z, xx)
        )

    def returned(i, xx):
        return remote(ret.at[i, xx], back.at[i, x], r_send.at[i, xx], r_recv.at[i, x], device(s, z, xx))

    def came_back(i, xx):
        return remote(ret.at[i, x], back.at[i, xx], r_send.at[i, xx], r_recv.at[i, xx], device(s, z, xx))

    def v_returned(i, xx):
        return remote(vret.at[i], vback.at[i, x], v_send.at[i, xx], v_recv.at[i, x], device(s, z, xx))

    def v_came_back(i, xx):
        return remote(vret.at[i], vback.at[i, xx], v_send.at[i, xx], v_recv.at[i, xx], device(s, z, xx))

    def onward(i):
        if i == 7:
            low, high = pl.ds(0, D // 2), pl.ds(D // 2, D // 2)
            return [
                remote(part.at[7, :, low], inc.at[5, :, low], p_send.at[5], p_recv.at[5], above),
                remote(part.at[7, :, high], inc.at[6, :, high], p_send.at[6], p_recv.at[6], below),
            ]
        if i > 2:
            to = above if i % 2 else below
            return [remote(part.at[i], inc.at[i - 2], p_send.at[i - 2], p_recv.at[i - 2], to)]
        to = device(s_prev, z + AWAY[i], x)
        return [remote(part.at[i], fin.at[i], f_send.at[i], f_recv.at[i], to)]

    def incoming(i):
        return onward(7)[i - 5] if i > 4 else onward(i + 2)[0]

    def g_summed(i):
        return remote(gpart.at[i], gparts.at[i], g_send.at[i], g_recv.at[i], device(s, z + AWAY[i], x))

    own_in = pltpu.make_async_copy(x_in.at[0], tok.at[0, 0], in_sem.at[0])
    own_grad = pltpu.make_async_copy(g_in.at[0], tok.at[0, 1], in_sem.at[1])
    w_copies = [
        pltpu.make_async_copy(wg_in.at[0], wgu.at[:, :, pl.ds(0, H)], in_sem.at[2]),
        pltpu.make_async_copy(wu_in.at[0], wgu.at[:, :, pl.ds(H, H)], in_sem.at[3]),
        pltpu.make_async_copy(wd_in.at[0], wd, in_sem.at[4]),
    ]
    own_in.start()
    own_grad.start()

    barrier = pltpu.get_barrier_semaphore()

    def greet(to):
        pl.semaphore_signal(barrier, inc=1, device_id=to, device_id_type=MESH)

    for k in range(1, NZ):
        greet(device(s, z + k, x))
    for xx in others:
        greet(device(s, z, xx))
    for k in (-1, 0, 1):
        greet(device(s_prev, z + k, x))
        greet(device(s_next, z + k, x))
    for c in w_copies:
        c.start()

    idt = ids_in[0].astype(F32)
    rtt = lev_in[0].astype(F32) / 256.0
    row = iota((TOK, TOK), 0)
    expert_of = ((row // 16) * 8 + row % 8).astype(F32)
    named = jnp.zeros((TOK, TOK), F32)
    route = jnp.zeros((TOK, TOK), F32)
    for k in range(TOPK):
        same = idt[k : k + 1, :] == expert_of
        named = jnp.where(same, 1.0, named)
        route = jnp.where(same, rtt[k : k + 1, :], route)
    before = jnp.where(iota((TOK, TOK), 0) < iota((TOK, TOK), 1), 1.0, 0.0).astype(BF16)
    slot = jnp.where(named > 0.5, dot(named.astype(BF16), before), -1.0)
    meta[0] = jnp.where(row % 16 < 8, slot, route).astype(BF16)

    def places(i):
        group = meta[i, pl.ds(pl.multiple_of(z * 16, 16), 16), :].astype(F32)
        place_of = iota((CAP, TOK), 0).astype(F32)
        ones, routes = [], []
        for k in range(ER):
            hit = group[k : k + 1, :] == place_of
            ones.append(jnp.where(hit, 1.0, 0.0))
            routes.append(jnp.where(hit, group[ER + k : ER + k + 1, :], 0.0))
        place[i] = jnp.concatenate(ones, axis=0).astype(BF16)
        place_w[i] = jnp.concatenate(routes, axis=0).astype(BF16)

    def chosen(i, h):
        if h == 0:
            places(i)
        which = place_w[i] if h else place[i]
        for n in range(0, D, 256):
            rows = dot(which, tok[i, h, :, n : n + 256]).astype(BF16)
            for q in range(NX):
                sel[i, q, h, :, n : n + 256] = rows[q * ROW : (q + 1) * ROW]

    def send_chosen(i, h):
        for xx in others:
            sent(i, h, xx).start()
        got[i, x, h] = sel[i, x, h]

    def pass_on(i, h):
        if h == 0:
            mt(i, i, above).wait_recv()
        ag(i, i, h, above).wait_recv()
        if i == 7 or (i == 5 and h == 0) or (i == 6 and h == 1):
            return
        to, dst = (below, above)[1 - i % 2], min(i + 2, 7)
        if h == 0:
            mt(i, dst, to).start()
        ag(i, dst, h, to).start()

    def select(i, h):
        chosen(i, h)
        send_chosen(i, h)

    def expert_rows(i):
        for xx in others:
            for h in range(2):
                arrived(i, h, xx).wait_recv()
        at = slice(i * SRC, (i + 1) * SRC)
        wide = [got[i, q, 0].astype(F32) for q in range(NX)]
        wide_w = [got[i, q, 1].astype(F32) for q in range(NX)]
        grads, vs = [], []
        for k in range(EL):
            mine = slice(k * CAP, (k + 1) * CAP)
            rows = jnp.concatenate([w[mine] for w in wide], axis=0).astype(BF16)
            weighted = jnp.concatenate([w[mine] for w in wide_w], axis=0).astype(BF16)
            xs[k, at, :] = rows
            ws[k, at, :] = weighted
            pre = dot(rows, wgu[k])
            gate, up = pre[:, :H], pre[:, H:]
            active_grad = dot_t(weighted, wd[k])
            sig = jax.nn.sigmoid(gate)
            silu = gate * sig
            active = (silu * up).astype(BF16)
            gate_grad = (active_grad * up * sig * (1.0 + gate * (1.0 - sig))).astype(BF16)
            up_grad = (active_grad * silu).astype(BF16)
            act[k, at, :] = active
            gug[k, at, 0:H] = gate_grad
            gug[k, at, H : 2 * H] = up_grad
            vs.append(jnp.sum(active.astype(F32) * active_grad, axis=1, keepdims=True))
            grads.append(jnp.concatenate([gate_grad, up_grad], axis=1))
        for n in range(0, D, 256):
            outs = [dot_t(grads[k], wgu[k, n : n + 256, :]) for k in range(EL)]
            for q in range(NX):
                piece = jnp.concatenate([o[q * CAP : (q + 1) * CAP] for o in outs], axis=0)
                ret[i, q, :, n : n + 256] = piece.astype(BF16)
        lines = []
        for q in range(NX):
            line = jnp.zeros((1, TOK), F32)
            for k in range(EL):
                at_lane = iota((CAP, TOK), 1) == iota((CAP, TOK), 0) + k * CAP
                line += jnp.sum(
                    jnp.where(at_lane, vs[k][q * CAP : (q + 1) * CAP], 0.0), axis=0, keepdims=True
                )
            lines.append(line)
        lines.append(jnp.zeros((8 - NX, TOK), F32))
        vret[i] = jnp.concatenate(lines, axis=0)
        back[i, x] = ret[i, x]
        vback[i, x] = vret[i]

    def send_back(i):
        for xx in others:
            returned(i, xx).start()
            v_returned(i, xx).start()

    def combine(i):
        for xx in others:
            came_back(i, xx).wait_recv()
            v_came_back(i, xx).wait_recv()
        if 0 < i < 7:
            incoming(i).wait_recv()
        one = place[i]
        for n in range(0, D, 256):
            rows = back[i, :, :, n : n + 256].reshape(ALL, 256)
            total = t_dot(one, rows)
            if 0 < i < 5 or (i == 5 and n < D // 2) or (i == 6 and n >= D // 2):
                total += inc[i, :, n : n + 256].astype(F32)
            part[i, :, n : n + 256] = total.astype(BF16)
        for c in onward(i):
            c.start()
        lines = []
        for q in range(NX):
            line = vback[i, q, pl.ds(x, 1), :]
            at_lane = iota((ROW, TOK), 1) == iota((ROW, TOK), 0)
            column = jnp.sum(jnp.where(at_lane, line, 0.0), axis=1, keepdims=True)
            spread = one[q * ROW : (q + 1) * ROW].astype(F32) * column
            for k in range(EL):
                lines.append(jnp.sum(spread[k * CAP : (k + 1) * CAP], axis=0, keepdims=True))
        summed = jnp.concatenate(lines, axis=0)
        if i:
            gpart[i] = summed
            g_summed(i).start()
        else:
            gparts[0] = summed

    def update(k, stage):
        if stage < 2:
            for m in range(stage * D // 2, (stage + 1) * D // 2, 256):
                new = t_dot(xs[k, :, m : m + 256], gug[k])
                gate_out[0, k, m : m + 256, :] = new[:, :H].astype(BF16)
                upw_out[0, k, m : m + 256, :] = new[:, H:].astype(BF16)
        else:
            down_out[0, k] = t_dot(act[k], ws[k]).astype(BF16)

    own_in.wait()
    own_grad.wait()
    chosen(0, 0)
    chosen(0, 1)
    pl.semaphore_wait(barrier, (NZ - 1) + (NX - 1) + 6)
    mt(0, 1, below).start()
    mt(0, 2, above).start()
    for h in range(2):
        ag(0, 1, h, below).start()
        ag(0, 2, h, above).start()
        send_chosen(0, h)

    def both(a, b, h):
        pass_on(a, h)
        pass_on(b, h)
        select(a, h)
        select(b, h)

    both(1, 2, 0)
    both(1, 2, 1)
    for c in w_copies:
        c.wait()
    expert_rows(0)
    both(3, 4, 0)
    expert_rows(1)
    both(3, 4, 1)
    expert_rows(2)
    both(5, 6, 0)
    expert_rows(3)
    pass_on(5, 1)
    pass_on(6, 1)
    select(5, 1)
    pass_on(7, 0)
    pass_on(7, 1)
    select(7, 0)
    select(7, 1)
    select(6, 1)
    expert_rows(4)
    expert_rows(5)
    expert_rows(7)
    send_back(7)
    send_back(5)
    expert_rows(6)
    for i in (6, 3, 4, 1, 2, 0):
        send_back(i)
    combine(7)
    update(0, 0)
    combine(5)
    update(0, 1)
    combine(6)
    update(0, 2)
    combine(3)
    update(1, 0)
    combine(4)
    update(1, 1)
    combine(1)
    update(1, 2)
    combine(2)
    combine(0)

    for i in range(1, NZ):
        g_summed(i).wait_recv()
    acc = jnp.zeros((TOPK, TOK), F32)
    idt = ids_in[0].astype(F32)
    for i in range(NZ):
        base = ((z + NZ - AWAY[i]) % NZ) * ER
        for k in range(ER):
            acc += jnp.where(idt == (base + k).astype(F32), gparts[i, k : k + 1, :], 0.0)
    rg_out[0] = (acc / (lev_in[0].astype(F32) / 256.0)).astype(BF16)

    for i in range(3):
        onward(i)[0].wait_recv()
    total = fin[0].astype(F32) + fin[1].astype(F32) + fin[2].astype(F32)
    up_out[0] = jnp.where(s == NS - 1, 0.0, total).astype(BF16)

    for i in range(NZ):
        if i:
            mt(0, i, above).wait_send()
            for h in range(2):
                ag(0, i, h, above).wait_send()
            g_summed(i).wait_send()
        for xx in others:
            for h in range(2):
                sent(i, h, xx).wait_send()
            returned(i, xx).wait_send()
            v_returned(i, xx).wait_send()
        for c in onward(i):
            c.wait_send()


def write_out(*refs):
    count = (len(refs) - 1) // 2
    copies = [pltpu.make_async_copy(refs[k], refs[count + k], refs[-1].at[k]) for k in range(count)]
    for c in copies:
        c.start()
    for c in copies:
        c.wait()


def body(inputs, out_grads, expert_ids, route_levels, w_gate, w_up, w_down):
    any_spec = pl.BlockSpec(memory_space=pl.ANY)
    vmem = pl.BlockSpec(memory_space=pltpu.VMEM)
    dma = pltpu.SemaphoreType.DMA
    flops = 2 * 8 * EL * NZ * SRC * D * H
    shapes = [(1, TOK, D), (1, TOPK, TOK), (1, EL, D, H), (1, EL, D, H), (1, EL, H, D)]
    results = pl.pallas_call(
        kernel,
        name="layer_backward",
        out_shape=[pltpu.VMEM(shape, BF16) for shape in shapes],
        in_specs=[any_spec, any_spec, vmem, vmem, any_spec, any_spec, any_spec],
        out_specs=[vmem] * 5,
        scratch_shapes=[
            pltpu.VMEM((NZ, 2, TOK, D), BF16),
            pltpu.VMEM((NZ, TOK, TOK), BF16),
            pltpu.VMEM((NZ, ALL, TOK), BF16),
            pltpu.VMEM((NZ, ALL, TOK), BF16),
            pltpu.VMEM((NZ, NX, 2, ROW, D), BF16),
            pltpu.VMEM((NZ, NX, 2, ROW, D), BF16),
            pltpu.VMEM((EL, D, 2 * H), BF16),
            pltpu.VMEM((EL, H, D), BF16),
            pltpu.VMEM((EL, NZ * SRC, D), BF16),
            pltpu.VMEM((EL, NZ * SRC, D), BF16),
            pltpu.VMEM((EL, NZ * SRC, H), BF16),
            pltpu.VMEM((EL, NZ * SRC, 2 * H), BF16),
            pltpu.VMEM((NZ, NX, ROW, D), BF16),
            pltpu.VMEM((NZ, NX, ROW, D), BF16),
            pltpu.VMEM((NZ, 8, TOK), F32),
            pltpu.VMEM((NZ, NX, 8, TOK), F32),
            pltpu.VMEM((NZ, TOK, D), BF16),
            pltpu.VMEM((NZ, TOK, D), BF16),
            pltpu.VMEM((3, TOK, D), BF16),
            pltpu.VMEM((NZ, ER, TOK), F32),
            pltpu.VMEM((NZ, ER, TOK), F32),
            dma((5,)),
            dma((NZ, 2)),
            dma((NZ, 2)),
            dma((NZ,)),
            dma((NZ,)),
            dma((NZ, NX, 2)),
            dma((NZ, NX, 2)),
            dma((NZ, NX)),
            dma((NZ, NX)),
            dma((NZ, NX)),
            dma((NZ, NX)),
            dma((NZ,)),
            dma((NZ,)),
            dma((3,)),
            dma((3,)),
            dma((NZ,)),
            dma((NZ,)),
        ],
        compiler_params=pltpu.CompilerParams(
            collective_id=0, has_side_effects=True, vmem_limit_bytes=56 * 1024 * 1024
        ),
        cost_estimate=pl.CostEstimate(flops=flops, bytes_accessed=12 << 20, transcendentals=EL * NZ * SRC * H),
    )(inputs, out_grads, jnp.swapaxes(expert_ids, 1, 2), jnp.swapaxes(route_levels, 1, 2), w_gate, w_up, w_down)
    upstream, route_grad, *updates = pl.pallas_call(
        write_out,
        name="write_out",
        out_shape=[jax.ShapeDtypeStruct(shape, BF16) for shape in shapes],
        in_specs=[any_spec] * 5,
        out_specs=[any_spec] * 5,
        scratch_shapes=[dma((5,))],
        compiler_params=pltpu.CompilerParams(vmem_limit_bytes=1 << 20),
        cost_estimate=pl.CostEstimate(flops=0, bytes_accessed=5 << 20, transcendentals=0),
    )(*results)
    return (upstream, jnp.swapaxes(route_grad, 1, 2), *updates)


def solution(mesh):
    rows = P("section", "expert", None)
    experts = P("section", "expert", None, None)
    return jax.shard_map(
        body,
        mesh=mesh,
        in_specs=(rows, rows, rows, rows, experts, experts, experts),
        out_specs=(rows, rows, experts, experts, experts),
        check_vma=False,
    )
```

```python
import jax
import jax.numpy as jnp
from jax import lax
from jax.experimental import pallas as pl
from jax.experimental.pallas import tpu as pltpu
from jax.sharding import PartitionSpec as P

NZ = 8
NX = 4
NS = 8
TOK = 128
TOPK = 8
D = 1024
CW = 256
DA = D - CW
H = 384
EL = 2
CAP = 24
ROW = EL * CAP
ER = EL * NX
ALL = NX * ROW
SRC = NX * CAP
AWAY = (0, 1, -1, 2, -2, 3, -3, 4)
MESH = pl.DeviceIdType.MESH
F32 = jnp.float32
BF16 = jnp.bfloat16


def dot(a, b):
    return jnp.dot(a, b, preferred_element_type=F32)


def dot_t(a, b):
    return lax.dot_general(a, b, (((1,), (1,)), ((), ())), preferred_element_type=F32)


def t_dot(a, b):
    return lax.dot_general(a, b, (((0,), (0,)), ((), ())), preferred_element_type=F32)


def iota(shape, dim):
    return lax.broadcasted_iota(jnp.int32, shape, dim)


def kernel(
    x_in, g_in, ids_in, lev_in, wg_in, wu_in, wd_in,
    up_out, rg_out, gate_out, upw_out, down_out,
    tok, meta, cx, mo, mx, mf, zs, gotc, place, place_w, sel, got, wgu, wd, xs, ws, act, gug, ret, back, vret, vback,
    part, inc, fin, gpart, gparts,
    in_sem, cx_send, cx_recv, mx_send, mx_recv, c_send, c_recv, ag_send, ag_recv, mt_send, mt_recv, s_send, s_recv, r_send, r_recv,
    v_send, v_recv, p_send, p_recv, f_send, f_recv, g_send, g_recv,
):
    s = lax.axis_index("section")
    e = lax.axis_index("expert")
    z = e // NX
    x = e % NX
    s_prev = (s + NS - 1) % NS
    s_next = (s + 1) % NS
    others = [(x + q) % NX for q in range(1, NX)]

    def device(section, zz, xx):
        return {"section": section, "expert": ((zz + NZ) % NZ) * NX + xx}

    below, above = device(s, z - 1, x), device(s, z + 1, x)

    def remote(src, dst, send, recv, to):
        return pltpu.make_async_remote_copy(
            src_ref=src, dst_ref=dst, send_sem=send, recv_sem=recv, device_id=to, device_id_type=MESH
        )

    def ag(src, dst, h, to):
        return remote(tok.at[src, h], tok.at[dst, h], ag_send.at[dst, h], ag_recv.at[dst, h], to)

    def mt(src, dst, to):
        return remote(meta.at[src], meta.at[dst], mt_send.at[dst], mt_recv.at[dst], to)

    def sent(i, h, xx):
        return remote(
            sel.at[i, xx, h], got.at[i, x, h], s_send.at[i, xx, h], s_recv.at[i, x, h], device(s, z, xx)
        )

    def arrived(i, h, xx):
        return remote(
            sel.at[i, x, h], got.at[i, xx, h], s_send.at[i, xx, h], s_recv.at[i, xx, h], device(s, z, xx)
        )

    def returned(i, xx):
        return remote(ret.at[i, xx], back.at[i, x], r_send.at[i, xx], r_recv.at[i, x], device(s, z, xx))

    def came_back(i, xx):
        return remote(ret.at[i, x], back.at[i, xx], r_send.at[i, xx], r_recv.at[i, xx], device(s, z, xx))

    def v_returned(i, xx):
        return remote(vret.at[i], vback.at[i, x], v_send.at[i, xx], v_recv.at[i, x], device(s, z, xx))

    def v_came_back(i, xx):
        return remote(vret.at[i], vback.at[i, xx], v_send.at[i, xx], v_recv.at[i, xx], device(s, z, xx))

    def onward(i):
        if i == 7:
            low, high = pl.ds(0, D // 2), pl.ds(D // 2, D // 2)
            return [
                remote(part.at[7, :, low], inc.at[5, :, low], p_send.at[5], p_recv.at[5], above),
                remote(part.at[7, :, high], inc.at[6, :, high], p_send.at[6], p_recv.at[6], below),
            ]
        if i > 2:
            to = above if i % 2 else below
            return [remote(part.at[i], inc.at[i - 2], p_send.at[i - 2], p_recv.at[i - 2], to)]
        to = device(s_prev, z + AWAY[i], x)
        return [remote(part.at[i], fin.at[i], f_send.at[i], f_recv.at[i], to)]

    def incoming(i):
        return onward(7)[i - 5] if i > 4 else onward(i + 2)[0]

    def g_summed(i):
        return remote(gpart.at[i], gparts.at[i], g_send.at[i], g_recv.at[i], device(s, z + AWAY[i], x))

    def cx_sent(xx):
        return remote(cx.at[x], cx.at[x], cx_send.at[xx], cx_recv.at[x], device(s, z, xx))

    def cx_arrived(xx):
        return remote(cx.at[xx], cx.at[xx], cx_send.at[xx], cx_recv.at[xx], device(s, z, xx))

    def mx_sent(xx):
        return remote(mo.at[xx], mx.at[x], mx_send.at[xx], mx_recv.at[x], device(s, z, xx))

    def mx_arrived(xx):
        return remote(mo.at[x], mx.at[xx], mx_send.at[xx], mx_recv.at[xx], device(s, z, xx))

    def crossed(i):
        return remote(zs.at[i], gotc.at[i], c_send.at[i], c_recv.at[i], device(s, z - AWAY[i], x))

    first, last = pl.ds(0, DA), pl.ds(DA, CW)
    own = [
        pltpu.make_async_copy(x_in.at[0, :, last], cx.at[x, 0], in_sem.at[5]),
        pltpu.make_async_copy(g_in.at[0, :, last], cx.at[x, 1], in_sem.at[6]),
        pltpu.make_async_copy(x_in.at[0, :, first], tok.at[0, 0], in_sem.at[0]),
        pltpu.make_async_copy(g_in.at[0, :, first], tok.at[0, 1], in_sem.at[1]),
    ]
    w_copies = [
        pltpu.make_async_copy(wg_in.at[0], wgu.at[:, :, pl.ds(0, H)], in_sem.at[2]),
        pltpu.make_async_copy(wu_in.at[0], wgu.at[:, :, pl.ds(H, H)], in_sem.at[3]),
        pltpu.make_async_copy(wd_in.at[0], wd, in_sem.at[4]),
    ]
    for c in own:
        c.start()

    barrier = pltpu.get_barrier_semaphore()

    def greet(to):
        pl.semaphore_signal(barrier, inc=1, device_id=to, device_id_type=MESH)

    for k in range(1, NZ):
        greet(device(s, z + k, x))
    for xx in others:
        greet(device(s, z, xx))
    for k in (-1, 0, 1):
        greet(device(s_prev, z + k, x))
        greet(device(s_next, z + k, x))
    for c in w_copies:
        c.start()

    idt = ids_in[0].astype(F32)
    rtt = lev_in[0].astype(F32) / 256.0
    row = iota((TOK, TOK), 0)
    expert_of = ((row // 16) * 8 + row % 8).astype(F32)
    named = jnp.zeros((TOK, TOK), F32)
    route = jnp.zeros((TOK, TOK), F32)
    for k in range(TOPK):
        same = idt[k : k + 1, :] == expert_of
        named = jnp.where(same, 1.0, named)
        route = jnp.where(same, rtt[k : k + 1, :], route)
    before = jnp.where(iota((TOK, TOK), 0) < iota((TOK, TOK), 1), 1.0, 0.0).astype(BF16)
    slot = jnp.where(named > 0.5, dot(named.astype(BF16), before), -1.0)
    table = jnp.where(row % 16 < 8, slot, route).astype(BF16)
    meta[0] = table
    taken = (row % 32) // 4 * 16 + (row % 4) // 2 * 8 + row // 32 * 2 + row % 2
    moved = dot(jnp.where(taken == iota((TOK, TOK), 1), 1.0, 0.0).astype(BF16), table).astype(BF16)
    for q in range(NX):
        mo[q] = moved[32 * q : 32 * q + 32]
    mx[x] = mo[x]

    def places(i):
        group = meta[i, pl.ds(pl.multiple_of(z * 16, 16), 16), :].astype(F32)
        place_of = iota((CAP, TOK), 0).astype(F32)
        ones, routes = [], []
        for k in range(ER):
            hit = group[k : k + 1, :] == place_of
            ones.append(jnp.where(hit, 1.0, 0.0))
            routes.append(jnp.where(hit, group[ER + k : ER + k + 1, :], 0.0))
        place[i] = jnp.concatenate(ones, axis=0).astype(BF16)
        place_w[i] = jnp.concatenate(routes, axis=0).astype(BF16)

    def chosen(i, h):
        if h == 0:
            places(i)
        which = place_w[i] if h else place[i]
        for n in range(0, DA, 256):
            m = min(n + 256, DA)
            rows = dot(which, tok[i, h, :, n:m]).astype(BF16)
            for q in range(NX):
                sel[i, q, h, :, n:m] = rows[q * ROW : (q + 1) * ROW]

    def send_chosen(i, h):
        for xx in others:
            sent(i, h, xx).start()
        got[i, x, h] = sel[i, x, h]

    def cross(q):
        mf[q] = mx[q].astype(F32)
        place_of = iota((CAP, TOK), 0).astype(F32)
        ones, routes = [], []
        for i in range(NZ):
            group = ((z + NZ - AWAY[i]) % NZ) * 4
            for k in range(EL):
                hit = mf[q, pl.ds(group + k, 1), :] == place_of
                ones.append(jnp.where(hit, 1.0, 0.0))
                routes.append(jnp.where(hit, mf[q, pl.ds(group + EL + k, 1), :], 0.0))
        for h, pieces in ((0, ones), (1, routes)):
            rows = dot(jnp.concatenate(pieces, axis=0).astype(BF16), cx[q, h]).astype(BF16)
            for i in range(NZ):
                zs[i, q, h] = rows[i * ROW : (i + 1) * ROW]

    def pass_on(i, h):
        if h == 0:
            mt(i, i, above).wait_recv()
        ag(i, i, h, above).wait_recv()
        if i == 7 or (i == 5 and h == 0) or (i == 6 and h == 1):
            return
        to, dst = (below, above)[1 - i % 2], min(i + 2, 7)
        if h == 0:
            mt(i, dst, to).start()
        ag(i, dst, h, to).start()

    def select(i, h):
        chosen(i, h)
        send_chosen(i, h)

    def expert_rows(i):
        for xx in others:
            for h in range(2):
                arrived(i, h, xx).wait_recv()
        if i:
            crossed(i).wait_recv()
        others_of = gotc if i else zs
        at = slice(i * SRC, (i + 1) * SRC)
        wide = [[got[i, q, h].astype(F32) for q in range(NX)] for h in range(2)]
        wide_c = [[others_of[i, q, h].astype(F32) for q in range(NX)] for h in range(2)]
        grads, vs = [], []
        for k in range(EL):
            mine = slice(k * CAP, (k + 1) * CAP)
            both_of = []
            for h, kept in ((0, xs), (1, ws)):
                part_a = jnp.concatenate([w[mine] for w in wide[h]], axis=0).astype(BF16)
                part_c = jnp.concatenate([w[mine] for w in wide_c[h]], axis=0).astype(BF16)
                kept[k, at, 0:DA] = part_a
                kept[k, at, DA:D] = part_c
                both_of.append(jnp.concatenate([part_a, part_c], axis=1))
            rows, weighted = both_of
            pre = dot(rows, wgu[k])
            gate, up = pre[:, :H], pre[:, H:]
            active_grad = dot_t(weighted, wd[k])
            sig = jax.nn.sigmoid(gate)
            silu = gate * sig
            active = (silu * up).astype(BF16)
            gate_grad = (active_grad * up * sig * (1.0 + gate * (1.0 - sig))).astype(BF16)
            up_grad = (active_grad * silu).astype(BF16)
            act[k, at, :] = active
            gug[k, at, 0:H] = gate_grad
            gug[k, at, H : 2 * H] = up_grad
            vs.append(jnp.sum(active.astype(F32) * active_grad, axis=1, keepdims=True))
            grads.append(jnp.concatenate([gate_grad, up_grad], axis=1))
        for n in range(0, D, 256):
            outs = [dot_t(grads[k], wgu[k, n : n + 256, :]) for k in range(EL)]
            for q in range(NX):
                piece = jnp.concatenate([o[q * CAP : (q + 1) * CAP] for o in outs], axis=0)
                ret[i, q, :, n : n + 256] = piece.astype(BF16)
        lines = []
        for q in range(NX):
            line = jnp.zeros((1, TOK), F32)
            for k in range(EL):
                at_lane = iota((CAP, TOK), 1) == iota((CAP, TOK), 0) + k * CAP
                line += jnp.sum(
                    jnp.where(at_lane, vs[k][q * CAP : (q + 1) * CAP], 0.0), axis=0, keepdims=True
                )
            lines.append(line)
        lines.append(jnp.zeros((8 - NX, TOK), F32))
        vret[i] = jnp.concatenate(lines, axis=0)
        back[i, x] = ret[i, x]
        vback[i, x] = vret[i]

    def send_back(i):
        for xx in others:
            returned(i, xx).start()
            v_returned(i, xx).start()

    def combine(i):
        for xx in others:
            came_back(i, xx).wait_recv()
            v_came_back(i, xx).wait_recv()
        if 0 < i < 7:
            incoming(i).wait_recv()
        one = place[i]
        for n in range(0, D, 256):
            rows = back[i, :, :, n : n + 256].reshape(ALL, 256)
            total = t_dot(one, rows)
            if 0 < i < 5 or (i == 5 and n < D // 2) or (i == 6 and n >= D // 2):
                total += inc[i, :, n : n + 256].astype(F32)
            part[i, :, n : n + 256] = total.astype(BF16)
        for c in onward(i):
            c.start()
        lines = []
        for q in range(NX):
            line = vback[i, q, pl.ds(x, 1), :]
            at_lane = iota((ROW, TOK), 1) == iota((ROW, TOK), 0)
            column = jnp.sum(jnp.where(at_lane, line, 0.0), axis=1, keepdims=True)
            spread = one[q * ROW : (q + 1) * ROW].astype(F32) * column
            for k in range(EL):
                lines.append(jnp.sum(spread[k * CAP : (k + 1) * CAP], axis=0, keepdims=True))
        summed = jnp.concatenate(lines, axis=0)
        if i:
            gpart[i] = summed
            g_summed(i).start()
        else:
            gparts[0] = summed

    def update(k, stage):
        if stage < 2:
            for m in range(stage * D // 2, (stage + 1) * D // 2, 256):
                new = t_dot(xs[k, :, m : m + 256], gug[k])
                gate_out[0, k, m : m + 256, :] = new[:, :H].astype(BF16)
                upw_out[0, k, m : m + 256, :] = new[:, H:].astype(BF16)
        else:
            down_out[0, k] = t_dot(act[k], ws[k]).astype(BF16)

    for c in own:
        c.wait()
    chosen(0, 0)
    chosen(0, 1)
    pl.semaphore_wait(barrier, (NZ - 1) + (NX - 1) + 6)
    for xx in others:
        mx_sent(xx).start()
        cx_sent(xx).start()
    mt(0, 1, below).start()
    mt(0, 2, above).start()
    for h in range(2):
        ag(0, 1, h, below).start()
        ag(0, 2, h, above).start()
        send_chosen(0, h)

    def both(a, b, h):
        pass_on(a, h)
        pass_on(b, h)
        select(a, h)
        select(b, h)

    both(1, 2, 0)
    for xx in others:
        mx_arrived(xx).wait_recv()
        cx_arrived(xx).wait_recv()
    cross(0)
    cross(1)
    pass_on(1, 1)
    pass_on(2, 1)
    select(1, 1)
    select(2, 1)
    cross(2)
    cross(3)
    for c in w_copies:
        c.wait()
    expert_rows(0)
    both(3, 4, 0)
    both(3, 4, 1)
    both(5, 6, 0)
    pass_on(5, 1)
    pass_on(6, 1)
    for i in (7, 5, 6, 3, 4, 1, 2):
        crossed(i).start()
    select(5, 1)
    pass_on(7, 0)
    pass_on(7, 1)
    select(7, 0)
    select(7, 1)
    select(6, 1)
    expert_rows(7)
    send_back(7)
    expert_rows(5)
    send_back(5)
    expert_rows(6)
    send_back(6)
    expert_rows(3)
    send_back(3)
    combine(7)
    expert_rows(4)
    send_back(4)
    combine(5)
    expert_rows(1)
    send_back(1)
    expert_rows(2)
    send_back(2)
    send_back(0)
    combine(6)
    update(0, 0)
    update(0, 1)
    combine(3)
    update(0, 2)
    update(1, 0)
    combine(4)
    update(1, 1)
    combine(1)
    update(1, 2)
    combine(2)
    combine(0)

    for i in range(1, NZ):
        g_summed(i).wait_recv()
    acc = jnp.zeros((TOPK, TOK), F32)
    idt = ids_in[0].astype(F32)
    for i in range(NZ):
        base = ((z + NZ - AWAY[i]) % NZ) * ER
        for k in range(ER):
            acc += jnp.where(idt == (base + k).astype(F32), gparts[i, k : k + 1, :], 0.0)
    rg_out[0] = (acc / (lev_in[0].astype(F32) / 256.0)).astype(BF16)

    for i in range(3):
        onward(i)[0].wait_recv()
    total = fin[0].astype(F32) + fin[1].astype(F32) + fin[2].astype(F32)
    up_out[0] = jnp.where(s == NS - 1, 0.0, total).astype(BF16)

    for i in range(NZ):
        if i:
            mt(0, i, above).wait_send()
            for h in range(2):
                ag(0, i, h, above).wait_send()
            g_summed(i).wait_send()
            crossed(i).wait_send()
        for xx in others:
            for h in range(2):
                sent(i, h, xx).wait_send()
            returned(i, xx).wait_send()
            v_returned(i, xx).wait_send()
        for c in onward(i):
            c.wait_send()
    for xx in others:
        cx_sent(xx).wait_send()
        mx_sent(xx).wait_send()


def write_out(*refs):
    count = (len(refs) - 1) // 2
    copies = [pltpu.make_async_copy(refs[k], refs[count + k], refs[-1].at[k]) for k in range(count)]
    for c in copies:
        c.start()
    for c in copies:
        c.wait()


def body(inputs, out_grads, expert_ids, route_levels, w_gate, w_up, w_down):
    any_spec = pl.BlockSpec(memory_space=pl.ANY)
    vmem = pl.BlockSpec(memory_space=pltpu.VMEM)
    dma = pltpu.SemaphoreType.DMA
    flops = 2 * 8 * EL * NZ * SRC * D * H
    shapes = [(1, TOK, D), (1, TOPK, TOK), (1, EL, D, H), (1, EL, D, H), (1, EL, H, D)]
    results = pl.pallas_call(
        kernel,
        name="layer_backward",
        out_shape=[pltpu.VMEM(shape, BF16) for shape in shapes],
        in_specs=[any_spec, any_spec, vmem, vmem, any_spec, any_spec, any_spec],
        out_specs=[vmem] * 5,
        scratch_shapes=[
            pltpu.VMEM((NZ, 2, TOK, DA), BF16),
            pltpu.VMEM((NZ, TOK, TOK), BF16),
            pltpu.VMEM((NX, 2, TOK, CW), BF16),
            pltpu.VMEM((NX, 32, TOK), BF16),
            pltpu.VMEM((NX, 32, TOK), BF16),
            pltpu.VMEM((NX, 32, TOK), F32),
            pltpu.VMEM((NZ, NX, 2, ROW, CW), BF16),
            pltpu.VMEM((NZ, NX, 2, ROW, CW), BF16),
            pltpu.VMEM((NZ, ALL, TOK), BF16),
            pltpu.VMEM((NZ, ALL, TOK), BF16),
            pltpu.VMEM((NZ, NX, 2, ROW, DA), BF16),
            pltpu.VMEM((NZ, NX, 2, ROW, DA), BF16),
            pltpu.VMEM((EL, D, 2 * H), BF16),
            pltpu.VMEM((EL, H, D), BF16),
            pltpu.VMEM((EL, NZ * SRC, D), BF16),
            pltpu.VMEM((EL, NZ * SRC, D), BF16),
            pltpu.VMEM((EL, NZ * SRC, H), BF16),
            pltpu.VMEM((EL, NZ * SRC, 2 * H), BF16),
            pltpu.VMEM((NZ, NX, ROW, D), BF16),
            pltpu.VMEM((NZ, NX, ROW, D), BF16),
            pltpu.VMEM((NZ, 8, TOK), F32),
            pltpu.VMEM((NZ, NX, 8, TOK), F32),
            pltpu.VMEM((NZ, TOK, D), BF16),
            pltpu.VMEM((NZ, TOK, D), BF16),
            pltpu.VMEM((3, TOK, D), BF16),
            pltpu.VMEM((NZ, ER, TOK), F32),
            pltpu.VMEM((NZ, ER, TOK), F32),
            dma((7,)),
            dma((NX,)),
            dma((NX,)),
            dma((NX,)),
            dma((NX,)),
            dma((NZ,)),
            dma((NZ,)),
            dma((NZ, 2)),
            dma((NZ, 2)),
            dma((NZ,)),
            dma((NZ,)),
            dma((NZ, NX, 2)),
            dma((NZ, NX, 2)),
            dma((NZ, NX)),
            dma((NZ, NX)),
            dma((NZ, NX)),
            dma((NZ, NX)),
            dma((NZ,)),
            dma((NZ,)),
            dma((3,)),
            dma((3,)),
            dma((NZ,)),
            dma((NZ,)),
        ],
        compiler_params=pltpu.CompilerParams(
            collective_id=0, has_side_effects=True, vmem_limit_bytes=56 * 1024 * 1024
        ),
        cost_estimate=pl.CostEstimate(flops=flops, bytes_accessed=12 << 20, transcendentals=EL * NZ * SRC * H),
    )(inputs, out_grads, jnp.swapaxes(expert_ids, 1, 2), jnp.swapaxes(route_levels, 1, 2), w_gate, w_up, w_down)
    upstream, route_grad, *updates = pl.pallas_call(
        write_out,
        name="write_out",
        out_shape=[jax.ShapeDtypeStruct(shape, BF16) for shape in shapes],
        in_specs=[any_spec] * 5,
        out_specs=[any_spec] * 5,
        scratch_shapes=[dma((5,))],
        compiler_params=pltpu.CompilerParams(vmem_limit_bytes=1 << 20),
        cost_estimate=pl.CostEstimate(flops=0, bytes_accessed=5 << 20, transcendentals=0),
    )(*results)
    return (upstream, jnp.swapaxes(route_grad, 1, 2), *updates)


def solution(mesh):
    rows = P("section", "expert", None)
    experts = P("section", "expert", None, None)
    return jax.shard_map(
        body,
        mesh=mesh,
        in_specs=(rows, rows, rows, rows, experts, experts, experts),
        out_specs=(rows, rows, experts, experts, experts),
        check_vma=False,
    )
```

```python
import jax
import jax.numpy as jnp
from jax import lax
from jax.experimental import pallas as pl
from jax.experimental.pallas import tpu as pltpu
from jax.sharding import PartitionSpec as P

NZ = 8
NX = 4
NS = 8
TOK = 128
TOPK = 8
D = 1024
CW = 256
DA = D - CW
H = 384
EL = 2
CAP = 24
NP = 2
PC = D // NP
ROW = EL * CAP
ER = EL * NX
ALL = NX * ROW
SRC = NX * CAP
AWAY = (0, 1, -1, 2, -2, 3, -3, 4)
MESH = pl.DeviceIdType.MESH
F32 = jnp.float32
BF16 = jnp.bfloat16


def dot(a, b):
    return jnp.dot(a, b, preferred_element_type=F32)


def dot_t(a, b):
    return lax.dot_general(a, b, (((1,), (1,)), ((), ())), preferred_element_type=F32)


def t_dot(a, b):
    return lax.dot_general(a, b, (((0,), (0,)), ((), ())), preferred_element_type=F32)


def iota(shape, dim):
    return lax.broadcasted_iota(jnp.int32, shape, dim)


def kernel(
    x_in, g_in, ids_in, lev_in, wg_in, wu_in, wd_in,
    up_out, rg_out, gate_out, upw_out, down_out,
    tok, meta, cx, mo, mx, mf, zs, gotc, place, place_w, sel, got, wgu, wd, xs, ws, act, gug, ret, back, vret, vback,
    part, inc, fin, gpart, gparts,
    in_sem, cx_send, cx_recv, mx_send, mx_recv, c_send, c_recv, ag_send, ag_recv, mt_send, mt_recv, s_send, s_recv, r_send, r_recv,
    v_send, v_recv, p_send, p_recv, f_send, f_recv, g_send, g_recv,
):
    s = lax.axis_index("section")
    e = lax.axis_index("expert")
    z = e // NX
    x = e % NX
    s_prev = (s + NS - 1) % NS
    s_next = (s + 1) % NS
    others = [(x + q) % NX for q in (2, 1, 3)]

    def device(section, zz, xx):
        return {"section": section, "expert": ((zz + NZ) % NZ) * NX + xx}

    below, above = device(s, z - 1, x), device(s, z + 1, x)

    def remote(src, dst, send, recv, to):
        return pltpu.make_async_remote_copy(
            src_ref=src, dst_ref=dst, send_sem=send, recv_sem=recv, device_id=to, device_id_type=MESH
        )

    def ag(src, dst, h, to):
        return remote(tok.at[src, h], tok.at[dst, h], ag_send.at[dst, h], ag_recv.at[dst, h], to)

    def mt(src, dst, to):
        return remote(meta.at[src], meta.at[dst], mt_send.at[dst], mt_recv.at[dst], to)

    def sent(i, h, xx):
        return remote(
            sel.at[i, xx, h], got.at[i, x, h], s_send.at[i, xx, h], s_recv.at[i, x, h], device(s, z, xx)
        )

    def arrived(i, h, xx):
        return remote(
            sel.at[i, x, h], got.at[i, xx, h], s_send.at[i, xx, h], s_recv.at[i, xx, h], device(s, z, xx)
        )

    def spans(i):
        return [(p, pl.ds(p * PC, PC)) for p in range(NP)] if i in (0, 1, 2) else [(0, pl.ds(0, D))]

    def returned(i, xx):
        return [
            remote(
                ret.at[i, xx, :, c], back.at[i, x, :, c], r_send.at[i, xx, p], r_recv.at[i, x, p],
                device(s, z, xx),
            )
            for p, c in spans(i)
        ]

    def came_back(i, xx):
        return [
            remote(
                ret.at[i, x, :, c], back.at[i, xx, :, c], r_send.at[i, xx, p], r_recv.at[i, xx, p],
                device(s, z, xx),
            )
            for p, c in spans(i)
        ]

    def v_returned(xx):
        return remote(vret, vback.at[x], v_send.at[xx], v_recv.at[x], device(s, z, xx))

    def v_came_back(xx):
        return remote(vret, vback.at[xx], v_send.at[xx], v_recv.at[xx], device(s, z, xx))

    def onward(i, p):
        cols = pl.ds(p * PC, PC)
        if i < 3:
            to = device(s_prev, z + AWAY[i], x)
            return remote(
                part.at[i, :, cols], fin.at[i, :, cols], f_send.at[i, p], f_recv.at[i, p], to
            )
        up = p < NP // 2 if i == 7 else i % 2 == 1
        dst = (5 if up else 6) if i == 7 else i - 2
        return remote(
            part.at[i, :, cols], inc.at[dst, :, cols], p_send.at[dst, p], p_recv.at[dst, p],
            above if up else below,
        )

    def pieces_in(i):
        if i == 5:
            return range(NP // 2)
        if i == 6:
            return range(NP // 2, NP)
        return range(NP) if 0 < i < 5 else ()

    def pieces(i):
        upward = i % 2 == 1 and i != 7
        return (*range(NP // 2, NP), *range(NP // 2)) if upward else range(NP)

    def g_summed(i):
        return remote(gpart.at[i], gparts.at[i], g_send.at[i], g_recv.at[i], device(s, z + AWAY[i], x))

    def cx_sent(xx):
        return remote(cx.at[x], cx.at[x], cx_send.at[xx], cx_recv.at[x], device(s, z, xx))

    def cx_arrived(xx):
        return remote(cx.at[xx], cx.at[xx], cx_send.at[xx], cx_recv.at[xx], device(s, z, xx))

    def mx_sent(xx):
        return remote(mo.at[xx], mx.at[x], mx_send.at[xx], mx_recv.at[x], device(s, z, xx))

    def mx_arrived(xx):
        return remote(mo.at[x], mx.at[xx], mx_send.at[xx], mx_recv.at[xx], device(s, z, xx))

    def crossed(i):
        return remote(zs.at[i], gotc.at[i], c_send.at[i], c_recv.at[i], device(s, z - AWAY[i], x))

    first, last = pl.ds(0, DA), pl.ds(DA, CW)
    own = [
        pltpu.make_async_copy(x_in.at[0, :, last], cx.at[x, 0], in_sem.at[5]),
        pltpu.make_async_copy(g_in.at[0, :, last], cx.at[x, 1], in_sem.at[6]),
        pltpu.make_async_copy(x_in.at[0, :, first], tok.at[0, 0], in_sem.at[0]),
        pltpu.make_async_copy(g_in.at[0, :, first], tok.at[0, 1], in_sem.at[1]),
    ]
    w_copies = [
        pltpu.make_async_copy(wg_in.at[0], wgu.at[:, :, pl.ds(0, H)], in_sem.at[2]),
        pltpu.make_async_copy(wu_in.at[0], wgu.at[:, :, pl.ds(H, H)], in_sem.at[3]),
        pltpu.make_async_copy(wd_in.at[0], wd, in_sem.at[4]),
    ]
    for c in own:
        c.start()

    barrier = pltpu.get_barrier_semaphore()

    def greet(to):
        pl.semaphore_signal(barrier, inc=1, device_id=to, device_id_type=MESH)

    for k in range(1, NZ):
        greet(device(s, z + k, x))
    for xx in others:
        greet(device(s, z, xx))
    for k in (-1, 0, 1):
        greet(device(s_prev, z + k, x))
        greet(device(s_next, z + k, x))
    for c in w_copies:
        c.start()

    idt = ids_in[0].astype(F32)
    rtt = lev_in[0].astype(F32) / 256.0
    row = iota((TOK, TOK), 0)
    expert_of = ((row // 16) * 8 + row % 8).astype(F32)
    named = jnp.zeros((TOK, TOK), F32)
    route = jnp.zeros((TOK, TOK), F32)
    for k in range(TOPK):
        same = idt[k : k + 1, :] == expert_of
        named = jnp.where(same, 1.0, named)
        route = jnp.where(same, rtt[k : k + 1, :], route)
    before = jnp.where(iota((TOK, TOK), 0) < iota((TOK, TOK), 1), 1.0, 0.0).astype(BF16)
    slot = jnp.where(named > 0.5, dot(named.astype(BF16), before), -1.0)
    table = jnp.where(row % 16 < 8, slot, route).astype(BF16)
    meta[0] = table
    taken = (row % 32) // 4 * 16 + (row % 4) // 2 * 8 + row // 32 * 2 + row % 2
    moved = dot(jnp.where(taken == iota((TOK, TOK), 1), 1.0, 0.0).astype(BF16), table).astype(BF16)
    for q in range(NX):
        mo[q] = moved[32 * q : 32 * q + 32]
    mx[x] = mo[x]

    def places(i):
        group = meta[i, pl.ds(pl.multiple_of(z * 16, 16), 16), :].astype(F32)
        place_of = iota((CAP, TOK), 0).astype(F32)
        ones, routes = [], []
        for k in range(ER):
            hit = group[k : k + 1, :] == place_of
            ones.append(jnp.where(hit, 1.0, 0.0))
            routes.append(jnp.where(hit, group[ER + k : ER + k + 1, :], 0.0))
        place[i] = jnp.concatenate(ones, axis=0).astype(BF16)
        place_w[i] = jnp.concatenate(routes, axis=0).astype(BF16)

    def chosen(i, h):
        if h == 0:
            places(i)
        which = place_w[i] if h else place[i]
        for n in range(0, DA, 256):
            m = min(n + 256, DA)
            rows = dot(which, tok[i, h, :, n:m]).astype(BF16)
            for q in range(NX):
                sel[i, q, h, :, n:m] = rows[q * ROW : (q + 1) * ROW]

    def send_chosen(i, h):
        for xx in others:
            sent(i, h, xx).start()
        got[i, x, h] = sel[i, x, h]

    def cross(q):
        mf[q] = mx[q].astype(F32)
        place_of = iota((CAP, TOK), 0).astype(F32)
        ones, routes = [], []
        for i in range(NZ):
            group = ((z + NZ - AWAY[i]) % NZ) * 4
            for k in range(EL):
                hit = mf[q, pl.ds(group + k, 1), :] == place_of
                ones.append(jnp.where(hit, 1.0, 0.0))
                routes.append(jnp.where(hit, mf[q, pl.ds(group + EL + k, 1), :], 0.0))
        for h, pieces in ((0, ones), (1, routes)):
            rows = dot(jnp.concatenate(pieces, axis=0).astype(BF16), cx[q, h]).astype(BF16)
            for i in range(NZ):
                zs[i, q, h] = rows[i * ROW : (i + 1) * ROW]

    def pass_on(i, h):
        if h == 0:
            mt(i, i, above).wait_recv()
        ag(i, i, h, above).wait_recv()
        if i == 7 or (i == 5 and h == 0) or (i == 6 and h == 1):
            return
        to, dst = (below, above)[1 - i % 2], min(i + 2, 7)
        if h == 0:
            mt(i, dst, to).start()
        ag(i, dst, h, to).start()

    def select(i, h):
        chosen(i, h)
        send_chosen(i, h)

    def expert_rows(i):
        for xx in others:
            for h in range(2):
                arrived(i, h, xx).wait_recv()
        if i:
            crossed(i).wait_recv()
        others_of = gotc if i else zs
        at = slice(i * SRC, (i + 1) * SRC)
        wide = [[got[i, q, h].astype(F32) for q in range(NX)] for h in range(2)]
        wide_c = [[others_of[i, q, h].astype(F32) for q in range(NX)] for h in range(2)]
        grads, vs = [], []
        for k in range(EL):
            mine = slice(k * CAP, (k + 1) * CAP)
            both_of = []
            for h, kept in ((0, xs), (1, ws)):
                part_a = jnp.concatenate([w[mine] for w in wide[h]], axis=0).astype(BF16)
                part_c = jnp.concatenate([w[mine] for w in wide_c[h]], axis=0).astype(BF16)
                kept[k, at, 0:DA] = part_a
                kept[k, at, DA:D] = part_c
                both_of.append(jnp.concatenate([part_a, part_c], axis=1))
            rows, weighted = both_of
            pre = dot(rows, wgu[k])
            gate, up = pre[:, :H], pre[:, H:]
            active_grad = dot_t(weighted, wd[k])
            sig = jax.nn.sigmoid(gate)
            silu = gate * sig
            active = (silu * up).astype(BF16)
            gate_grad = (active_grad * up * sig * (1.0 + gate * (1.0 - sig))).astype(BF16)
            up_grad = (active_grad * silu).astype(BF16)
            act[k, at, :] = active
            gug[k, at, 0:H] = gate_grad
            gug[k, at, H : 2 * H] = up_grad
            vs.append(jnp.sum(active.astype(F32) * active_grad, axis=1, keepdims=True))
            grads.append(jnp.concatenate([gate_grad, up_grad], axis=1))
        for n in range(0, D, 256):
            outs = [dot_t(grads[k], wgu[k, n : n + 256, :]) for k in range(EL)]
            for q in range(NX):
                piece = jnp.concatenate([o[q * CAP : (q + 1) * CAP] for o in outs], axis=0)
                ret[i, q, :, n : n + 256] = piece.astype(BF16)
        lines = []
        for q in range(NX):
            line = jnp.zeros((1, TOK), F32)
            for k in range(EL):
                at_lane = iota((CAP, TOK), 1) == iota((CAP, TOK), 0) + k * CAP
                line += jnp.sum(
                    jnp.where(at_lane, vs[k][q * CAP : (q + 1) * CAP], 0.0), axis=0, keepdims=True
                )
            lines.append(line)
        lines.append(jnp.zeros((8 - NX, TOK), F32))
        vret[i] = jnp.concatenate(lines, axis=0)
        back[i, x] = ret[i, x]
        vback[x, i] = vret[i]

    def send_back(i):
        for p in range(len(spans(i))):
            for xx in others:
                returned(i, xx)[p].start()

    def send_v():
        for xx in others:
            v_returned(xx).start()

    def combine(i):
        one = place[i]
        for count, p in enumerate(pieces(i)):
            if count == 0 or len(spans(i)) > 1:
                for xx in others:
                    came_back(i, xx)[p if len(spans(i)) > 1 else 0].wait_recv()
            if p in pieces_in(i):
                onward(7 if i > 4 else i + 2, p).wait_recv()
            for n in range(p * PC, (p + 1) * PC, 256):
                rows = back[i, :, :, n : n + 256].reshape(ALL, 256)
                total = t_dot(one, rows)
                if p in pieces_in(i):
                    total += inc[i, :, n : n + 256].astype(F32)
                part[i, :, n : n + 256] = total.astype(BF16)
            onward(i, p).start()
    def routes():
        for xx in others:
            v_came_back(xx).wait_recv()
        for i in range(1 - NZ, 1):
            i = -i
            one = place[i]
            lines = []
            for q in range(NX):
                line = vback[q, i, pl.ds(x, 1), :]
                at_lane = iota((ROW, TOK), 1) == iota((ROW, TOK), 0)
                column = jnp.sum(jnp.where(at_lane, line, 0.0), axis=1, keepdims=True)
                spread = one[q * ROW : (q + 1) * ROW].astype(F32) * column
                for k in range(EL):
                    lines.append(jnp.sum(spread[k * CAP : (k + 1) * CAP], axis=0, keepdims=True))
            summed = jnp.concatenate(lines, axis=0)
            if i:
                gpart[i] = summed
                g_summed(i).start()
            else:
                gparts[0] = summed

    def update(k, stage):
        if stage < 2:
            for m in range(stage * D // 2, (stage + 1) * D // 2, 256):
                new = t_dot(xs[k, :, m : m + 256], gug[k])
                gate_out[0, k, m : m + 256, :] = new[:, :H].astype(BF16)
                upw_out[0, k, m : m + 256, :] = new[:, H:].astype(BF16)
        else:
            down_out[0, k] = t_dot(act[k], ws[k]).astype(BF16)

    for c in own:
        c.wait()
    chosen(0, 0)
    chosen(0, 1)
    pl.semaphore_wait(barrier, (NZ - 1) + (NX - 1) + 6)
    for xx in others:
        mx_sent(xx).start()
        cx_sent(xx).start()
    mt(0, 1, below).start()
    mt(0, 2, above).start()
    for h in range(2):
        ag(0, 1, h, below).start()
        ag(0, 2, h, above).start()
        send_chosen(0, h)

    def both(a, b, h):
        pass_on(a, h)
        pass_on(b, h)
        select(a, h)
        select(b, h)

    both(1, 2, 0)
    for xx in others:
        mx_arrived(xx).wait_recv()
        cx_arrived(xx).wait_recv()
    cross(0)
    cross(1)
    pass_on(1, 1)
    pass_on(2, 1)
    select(1, 1)
    select(2, 1)
    cross(2)
    cross(3)
    for c in w_copies:
        c.wait()
    expert_rows(0)
    both(3, 4, 0)
    both(3, 4, 1)
    both(5, 6, 0)
    pass_on(5, 1)
    pass_on(6, 1)
    for i in (7, 5, 6, 3, 4, 1, 2):
        crossed(i).start()
    select(5, 1)
    pass_on(7, 0)
    pass_on(7, 1)
    select(7, 0)
    select(7, 1)
    select(6, 1)
    expert_rows(7)
    send_back(7)
    expert_rows(5)
    send_back(5)
    expert_rows(6)
    send_back(6)
    combine(7)
    expert_rows(3)
    send_back(3)
    expert_rows(4)
    send_back(4)
    combine(5)
    expert_rows(1)
    send_back(1)
    expert_rows(2)
    send_v()
    send_back(2)
    send_back(0)
    combine(6)
    update(0, 0)
    update(0, 1)
    combine(3)
    update(0, 2)
    update(1, 0)
    combine(4)
    update(1, 1)
    combine(1)
    update(1, 2)
    combine(2)
    combine(0)
    routes()

    for i in range(1, NZ):
        g_summed(i).wait_recv()
    acc = jnp.zeros((TOPK, TOK), F32)
    idt = ids_in[0].astype(F32)
    for i in range(NZ):
        base = ((z + NZ - AWAY[i]) % NZ) * ER
        for k in range(ER):
            acc += jnp.where(idt == (base + k).astype(F32), gparts[i, k : k + 1, :], 0.0)
    rg_out[0] = (acc / (lev_in[0].astype(F32) / 256.0)).astype(BF16)

    for i in range(3):
        for p in range(NP):
            onward(i, p).wait_recv()
    total = fin[0].astype(F32) + fin[1].astype(F32) + fin[2].astype(F32)
    up_out[0] = jnp.where(s == NS - 1, 0.0, total).astype(BF16)

    for i in range(NZ):
        if i:
            mt(0, i, above).wait_send()
            for h in range(2):
                ag(0, i, h, above).wait_send()
            g_summed(i).wait_send()
            crossed(i).wait_send()
        for xx in others:
            for h in range(2):
                sent(i, h, xx).wait_send()
            for c in returned(i, xx):
                c.wait_send()
        for p in range(NP):
            onward(i, p).wait_send()
    for xx in others:
        cx_sent(xx).wait_send()
        v_returned(xx).wait_send()
        mx_sent(xx).wait_send()


def write_out(*refs):
    count = (len(refs) - 1) // 2
    copies = [pltpu.make_async_copy(refs[k], refs[count + k], refs[-1].at[k]) for k in range(count)]
    for c in copies:
        c.start()
    for c in copies:
        c.wait()


def body(inputs, out_grads, expert_ids, route_levels, w_gate, w_up, w_down):
    any_spec = pl.BlockSpec(memory_space=pl.ANY)
    vmem = pl.BlockSpec(memory_space=pltpu.VMEM)
    dma = pltpu.SemaphoreType.DMA
    flops = 2 * 8 * EL * NZ * SRC * D * H
    shapes = [(1, TOK, D), (1, TOPK, TOK), (1, EL, D, H), (1, EL, D, H), (1, EL, H, D)]
    results = pl.pallas_call(
        kernel,
        name="layer_backward",
        out_shape=[pltpu.VMEM(shape, BF16) for shape in shapes],
        in_specs=[any_spec, any_spec, vmem, vmem, any_spec, any_spec, any_spec],
        out_specs=[vmem] * 5,
        scratch_shapes=[
            pltpu.VMEM((NZ, 2, TOK, DA), BF16),
            pltpu.VMEM((NZ, TOK, TOK), BF16),
            pltpu.VMEM((NX, 2, TOK, CW), BF16),
            pltpu.VMEM((NX, 32, TOK), BF16),
            pltpu.VMEM((NX, 32, TOK), BF16),
            pltpu.VMEM((NX, 32, TOK), F32),
            pltpu.VMEM((NZ, NX, 2, ROW, CW), BF16),
            pltpu.VMEM((NZ, NX, 2, ROW, CW), BF16),
            pltpu.VMEM((NZ, ALL, TOK), BF16),
            pltpu.VMEM((NZ, ALL, TOK), BF16),
            pltpu.VMEM((NZ, NX, 2, ROW, DA), BF16),
            pltpu.VMEM((NZ, NX, 2, ROW, DA), BF16),
            pltpu.VMEM((EL, D, 2 * H), BF16),
            pltpu.VMEM((EL, H, D), BF16),
            pltpu.VMEM((EL, NZ * SRC, D), BF16),
            pltpu.VMEM((EL, NZ * SRC, D), BF16),
            pltpu.VMEM((EL, NZ * SRC, H), BF16),
            pltpu.VMEM((EL, NZ * SRC, 2 * H), BF16),
            pltpu.VMEM((NZ, NX, ROW, D), BF16),
            pltpu.VMEM((NZ, NX, ROW, D), BF16),
            pltpu.VMEM((NZ, 8, TOK), F32),
            pltpu.VMEM((NX, NZ, 8, TOK), F32),
            pltpu.VMEM((NZ, TOK, D), BF16),
            pltpu.VMEM((NZ, TOK, D), BF16),
            pltpu.VMEM((3, TOK, D), BF16),
            pltpu.VMEM((NZ, ER, TOK), F32),
            pltpu.VMEM((NZ, ER, TOK), F32),
            dma((7,)),
            dma((NX,)),
            dma((NX,)),
            dma((NX,)),
            dma((NX,)),
            dma((NZ,)),
            dma((NZ,)),
            dma((NZ, 2)),
            dma((NZ, 2)),
            dma((NZ,)),
            dma((NZ,)),
            dma((NZ, NX, 2)),
            dma((NZ, NX, 2)),
            dma((NZ, NX, NP)),
            dma((NZ, NX, NP)),
            dma((NX,)),
            dma((NX,)),
            dma((NZ, NP)),
            dma((NZ, NP)),
            dma((3, NP)),
            dma((3, NP)),
            dma((NZ,)),
            dma((NZ,)),
        ],
        compiler_params=pltpu.CompilerParams(
            collective_id=0, has_side_effects=True, vmem_limit_bytes=56 * 1024 * 1024
        ),
        cost_estimate=pl.CostEstimate(flops=flops, bytes_accessed=12 << 20, transcendentals=EL * NZ * SRC * H),
    )(inputs, out_grads, jnp.swapaxes(expert_ids, 1, 2), jnp.swapaxes(route_levels, 1, 2), w_gate, w_up, w_down)
    upstream, route_grad, *updates = pl.pallas_call(
        write_out,
        name="write_out",
        out_shape=[jax.ShapeDtypeStruct(shape, BF16) for shape in shapes],
        in_specs=[any_spec] * 5,
        out_specs=[any_spec] * 5,
        scratch_shapes=[dma((5,))],
        compiler_params=pltpu.CompilerParams(vmem_limit_bytes=1 << 20),
        cost_estimate=pl.CostEstimate(flops=0, bytes_accessed=5 << 20, transcendentals=0),
    )(*results)
    return (upstream, jnp.swapaxes(route_grad, 1, 2), *updates)


def solution(mesh):
    rows = P("section", "expert", None)
    experts = P("section", "expert", None, None)
    return jax.shard_map(
        body,
        mesh=mesh,
        in_specs=(rows, rows, rows, rows, experts, experts, experts),
        out_specs=(rows, rows, experts, experts, experts),
        check_vma=False,
    )
```
